128 devices in a mesh: dp: 1, tp: 128 (over z, y, x, core).
Axes of the slice: x: 4, y: 4, z: 4, core: 2. Of those that a mesh axis runs over, the one named last changes fastest.
Arguments:
- queries: bfloat16 [2048, 768], P(('dp', 'tp'))
- w_first: bfloat16 [768, 768], replicated
- w_second: bfloat16 [768, 128], replicated
- catalogue: bfloat16 [1048576, 128], P('tp')
- log_q: float32 [1048576], P('tp')
- labels: int32 [2048], P(('dp', 'tp'))
Outputs:
- output 1: float32 [1], P('dp')
- output 2: bfloat16 [1048576, 128], P(('dp', 'tp'))
- output 3: bfloat16 [768, 768], P('dp')
- output 4: bfloat16 [768, 128], P('dp')
All inputs are finite; a program needn't handle non-finite values.
Results may differ from the reference program's by a relative error of at most 0.00441204.
Values are sent between devices in bfloat16 or wider.
A program may use at most 1 GiB of HBM per device.

```python
import math
import jax
import jax.numpy as jnp
from jax import lax

QUERIES = 2048
ROW_BLOCK = 16
IN_DIM = 768
HID_DIM = 768
EMB_DIM = 128
NUM_ITEMS = 1048576


def setup_inputs(seed: int = 0, part: int = 0) -> dict:
    base_key = jax.random.key(seed)
    shared_keys = jax.random.split(base_key, 4)
    part_keys = jax.random.split(jax.random.fold_in(base_key, part), 2)
    queries = jax.random.normal(part_keys[0], (QUERIES, IN_DIM), jnp.float32).astype(jnp.bfloat16)
    w_first = (jax.random.normal(shared_keys[0], (IN_DIM, HID_DIM), jnp.float32) * (1.0 / IN_DIM) ** 0.5).astype(jnp.bfloat16)
    w_second = (jax.random.normal(shared_keys[1], (HID_DIM, EMB_DIM), jnp.float32) * (2.0 / HID_DIM) ** 0.5).astype(jnp.bfloat16)
    catalogue = (jax.random.normal(shared_keys[2], (NUM_ITEMS, EMB_DIM), jnp.float32) * (36.0 / EMB_DIM) ** 0.5).astype(jnp.bfloat16)
    log_q = jax.random.normal(shared_keys[3], (NUM_ITEMS,), jnp.float32) - math.log(NUM_ITEMS)
    labels = jax.random.randint(part_keys[1], (QUERIES,), 0, NUM_ITEMS, jnp.int32)
    return {"queries": queries, "w_first": w_first, "w_second": w_second, "catalogue": catalogue, "log_q": log_q, "labels": labels}


def reference(queries, w_first, w_second, catalogue, log_q, labels):
    pre_act = jnp.dot(queries, w_first, preferred_element_type=jnp.float32)
    hidden = jnp.maximum(pre_act, 0.0).astype(jnp.bfloat16)
    query_emb = jnp.dot(hidden, w_second, preferred_element_type=jnp.float32).astype(jnp.bfloat16)
    num_blocks = QUERIES // ROW_BLOCK
    item_ids = jnp.arange(NUM_ITEMS, dtype=jnp.int32)

    def block_step(grad_items, block_in):
        block_rows, row_labels = block_in
        logits = jnp.dot(block_rows, catalogue.T, preferred_element_type=jnp.float32) - log_q[None, :]
        row_max = jnp.max(logits, axis=1, keepdims=True)
        exp_all = jnp.exp(logits - row_max)
        sum_exp = jnp.sum(exp_all, axis=1, keepdims=True)
        label_hit = item_ids[None, :] == row_labels[:, None]
        target = jnp.sum(jnp.where(label_hit, logits, 0.0), axis=1)
        losses = row_max[:, 0] + jnp.log(sum_exp[:, 0]) - target
        soft_prob = exp_all / sum_exp
        grad_logits = (jnp.where(label_hit, soft_prob - 1.0, soft_prob) / QUERIES).astype(jnp.bfloat16)
        grad_items = grad_items + jnp.dot(grad_logits.T, block_rows, preferred_element_type=jnp.float32)
        grad_rows = jnp.dot(grad_logits, catalogue, preferred_element_type=jnp.float32)
        return grad_items, (losses, grad_rows)

    init_items = jnp.zeros((NUM_ITEMS, EMB_DIM), jnp.float32)
    grad_items, (losses, grad_rows) = lax.scan(block_step, init_items, (query_emb.reshape(num_blocks, ROW_BLOCK, EMB_DIM), labels.reshape(num_blocks, ROW_BLOCK)))
    mean_loss = jnp.mean(losses).reshape(1)
    grad_emb = grad_rows.reshape(QUERIES, EMB_DIM).astype(jnp.bfloat16)
    grad_second = jnp.dot(hidden.T, grad_emb, preferred_element_type=jnp.float32).astype(jnp.bfloat16)
    grad_hidden = jnp.dot(grad_emb, w_second.T, preferred_element_type=jnp.float32)
    grad_pre = jnp.where(pre_act > 0.0, grad_hidden, 0.0).astype(jnp.bfloat16)
    grad_first = jnp.dot(queries.T, grad_pre, preferred_element_type=jnp.float32).astype(jnp.bfloat16)
    return mean_loss, grad_items.astype(jnp.bfloat16), grad_first, grad_second
```

```python
import jax
import jax.numpy as jnp
from jax import lax
from jax.experimental import pallas as pl
from jax.experimental.pallas import tpu as pltpu
from jax.sharding import PartitionSpec as P

MESH = pl.DeviceIdType.MESH
DMA = pltpu.SemaphoreType.DMA


def peer(index):
    return {"tp": index}


def entry_barrier(me, n):
    barrier = pltpu.get_barrier_semaphore()

    @pl.loop(1, n)
    def _(k):
        pl.semaphore_signal(barrier, inc=1, device_id=peer(lax.rem(me + k, n)), device_id_type=MESH)

    pl.semaphore_wait(barrier, n - 1)


def drain(ref, sem):
    pltpu.make_async_copy(ref, ref, sem).wait()


def gather_kernel(n, emb_ref, lab_ref, q_ref, emb_all, lab_all, q_all, sems):
    me = lax.axis_index("tp")
    core, chip, chips = lax.rem(me, 2), me // 2, n // 2
    entry_barrier(me, n)
    emb_all[pl.ds(me, 1)] = emb_ref[...][None]
    lab_all[pl.ds(me, 1)] = lab_ref[...]
    q_all[core, pl.ds(chip, 1)] = q_ref[...][None]

    @pl.loop(1, n)
    def _(k):
        to = peer(lax.rem(me + k, n))
        pltpu.make_async_remote_copy(emb_ref, emb_all.at[me], sems.at[0], sems.at[1], device_id=to, device_id_type=MESH).start()
        pltpu.make_async_remote_copy(lab_ref.at[0], lab_all.at[me], sems.at[2], sems.at[3], device_id=to, device_id_type=MESH).start()

    @pl.loop(1, chips)
    def _(k):
        to = peer(lax.rem(chip + k, chips) * 2 + core)
        pltpu.make_async_remote_copy(q_ref, q_all.at[core, chip], sems.at[4], sems.at[5], device_id=to, device_id_type=MESH).start()

    for ref, s in ((emb_all.at[pl.ds(0, n - 1)], 0), (lab_all.at[pl.ds(0, n - 1)], 2), (q_all.at[0, pl.ds(0, chips - 1)], 4)):
        drain(ref, sems.at[s])
        drain(ref, sems.at[s + 1])
    swap = pltpu.make_async_remote_copy(q_all.at[core], q_all.at[core], sems.at[6], sems.at[7], device_id=peer(chip * 2 + 1 - core), device_id_type=MESH)
    swap.start()
    swap.wait_send()
    drain(q_all.at[0], sems.at[7])


def stats_kernel(n, part_ref, out_all, got, mine, sems):
    me = lax.axis_index("tp")
    entry_barrier(me, n)

    @pl.loop(1, n)
    def _(k):
        p = lax.rem(me + k, n)
        pltpu.make_async_remote_copy(part_ref.at[p], got.at[me], sems.at[0], sems.at[1], device_id=peer(p), device_id_type=MESH).start()

    got[pl.ds(me, 1)] = part_ref[pl.ds(me, 1)]
    w = got.at[pl.ds(0, n - 1)]
    drain(w, sems.at[0])
    drain(w, sems.at[1])
    top = jnp.max(got[:, 0:1, :], axis=0, keepdims=True)
    total = jnp.sum(got[:, 1:2, :] * jnp.exp(got[:, 0:1, :] - top), axis=0, keepdims=True)
    target = jnp.sum(got[:, 2:3, :], axis=0, keepdims=True)
    mine[:, 0:1, :] = top
    mine[:, 1:2, :] = total
    mine[:, 2:3, :] = target
    mine[:, 3:8, :] = jnp.zeros((1, 5, 128), jnp.float32)
    out_all[pl.ds(me, 1)] = mine[...]

    @pl.loop(1, n)
    def _(k):
        p = lax.rem(me + k, n)
        pltpu.make_async_remote_copy(mine.at[0], out_all.at[me], sems.at[2], sems.at[3], device_id=peer(p), device_id_type=MESH).start()

    w = out_all.at[pl.ds(0, n - 1)]
    drain(w, sems.at[2])
    drain(w, sems.at[3])


def grad_kernel(n, part_ref, out_all, got, mine, sems):
    me = lax.axis_index("tp")
    entry_barrier(me, n)

    @pl.loop(1, n)
    def _(k):
        p = lax.rem(me + k, n)
        pltpu.make_async_remote_copy(part_ref.at[p], got.at[me], sems.at[0], sems.at[1], device_id=peer(p), device_id_type=MESH).start()

    got[pl.ds(me, 1)] = part_ref[pl.ds(me, 1)]
    w = got.at[pl.ds(0, n - 1)]
    drain(w, sems.at[0])
    drain(w, sems.at[1])
    mine[...] = jnp.sum(got[...], axis=0).astype(jnp.bfloat16)
    out_all[pl.ds(me, 1)] = mine[...][None]

    @pl.loop(1, n)
    def _(k):
        p = lax.rem(me + k, n)
        pltpu.make_async_remote_copy(mine, out_all.at[me], sems.at[2], sems.at[3], device_id=peer(p), device_id_type=MESH).start()

    w = out_all.at[pl.ds(0, n - 1)]
    drain(w, sems.at[2])
    drain(w, sems.at[3])


VMEM = pl.BlockSpec(memory_space=pltpu.VMEM)


def comm_call(kernel, n, name, collective_id, outs, scratch, sems, ins):
    import functools

    return pl.pallas_call(
        functools.partial(kernel, n),
        name=name,
        out_shape=outs,
        in_specs=[VMEM] * len(ins),
        out_specs=jax.tree.map(lambda _: VMEM, outs),
        scratch_shapes=scratch + [DMA((sems,))],
        compiler_params=pltpu.CompilerParams(collective_id=collective_id, has_side_effects=True, vmem_limit_bytes=40 << 20),
    )(*ins)


def solution(mesh):
    n = mesh.shape["tp"]
    f32, bf16 = jnp.float32, jnp.bfloat16

    def local_step(queries, w_first, w_second, catalogue, log_q, labels):
        rows = queries.shape[0]
        items_local = catalogue.shape[0]
        shard_index = lax.axis_index("tp")
        pre_act = jnp.dot(queries, w_first, preferred_element_type=f32)
        hidden = jnp.maximum(pre_act, 0.0).astype(bf16)
        query_emb = jnp.dot(hidden, w_second, preferred_element_type=f32).astype(bf16)
        lab_pad = jnp.pad(labels, (0, 128 - rows)).reshape(1, 1, 128)
        emb_all, lab_all, q_all = comm_call(
            gather_kernel, n, "gather", 0,
            (jax.ShapeDtypeStruct((n, rows, 128), bf16), jax.ShapeDtypeStruct((n, 1, 128), jnp.int32), jax.ShapeDtypeStruct((2, n // 2, rows, queries.shape[1]), bf16)),
            [], 8, (query_emb, lab_pad, queries))
        emb_all = emb_all.reshape(n * rows, 128)
        q_all = q_all.transpose(1, 0, 2, 3).reshape(n * rows, -1)
        labels_all = lab_all[:, 0, :rows].reshape(n * rows)
        total_rows = n * rows
        logits = lax.dot_general(emb_all, catalogue, (((1,), (1,)), ((), ())), preferred_element_type=f32) - log_q[None, :]
        local_max = jnp.max(logits, axis=1)
        local_ids = labels_all - shard_index * items_local
        label_hit = lax.broadcasted_iota(jnp.int32, (1, items_local), 1) == local_ids[:, None]
        local_target = jnp.sum(jnp.where(label_hit, logits, 0.0), axis=1)
        exp_local = jnp.exp(logits - local_max[:, None])
        local_sum = jnp.sum(exp_local, axis=1)
        stats = jnp.stack([local_max, local_sum, local_target]).reshape(3, n, rows).transpose(1, 0, 2)
        stats = jnp.pad(stats, ((0, 0), (0, 5), (0, 128 - rows)))
        stats_all = comm_call(stats_kernel, n, "stats", 1, jax.ShapeDtypeStruct((n, 8, 128), f32),
                              [pltpu.VMEM((n, 8, 128), f32), pltpu.VMEM((1, 8, 128), f32)], 4, (stats,))
        row_max, sum_exp, target = (stats_all[:, i, :rows].reshape(total_rows) for i in range(3))
        mean_loss = jnp.mean(row_max + jnp.log(sum_exp) - target).reshape(1)
        soft_prob = exp_local * (jnp.exp(local_max - row_max) / sum_exp)[:, None]
        grad_logits = (jnp.where(label_hit, soft_prob - 1.0, soft_prob) / total_rows).astype(bf16)
        grad_items = lax.dot_general(grad_logits, emb_all, (((0,), (0,)), ((), ())), preferred_element_type=f32).astype(bf16)
        emb_part = jnp.dot(grad_logits, catalogue, preferred_element_type=f32)
        grad_emb = comm_call(grad_kernel, n, "grads", 2, jax.ShapeDtypeStruct((n, rows, 128), bf16),
                             [pltpu.VMEM((n, rows, 128), f32), pltpu.VMEM((rows, 128), bf16)], 4, (emb_part.reshape(n, rows, 128),))
        grad_emb = grad_emb.reshape(total_rows, 128)
        pre_all = jnp.dot(q_all, w_first, preferred_element_type=f32)
        hid_all = jnp.maximum(pre_all, 0.0).astype(bf16)
        grad_second = lax.dot_general(hid_all, grad_emb, (((0,), (0,)), ((), ())), preferred_element_type=f32).astype(bf16)
        grad_hidden = lax.dot_general(grad_emb, w_second, (((1,), (1,)), ((), ())), preferred_element_type=f32)
        grad_pre = jnp.where(pre_all > 0.0, grad_hidden, 0.0).astype(bf16)
        grad_first = lax.dot_general(q_all, grad_pre, (((0,), (0,)), ((), ())), preferred_element_type=f32).astype(bf16)
        return mean_loss, grad_items, grad_first, grad_second

    row_spec = P(("dp", "tp"), None)
    return jax.shard_map(local_step, mesh=mesh, in_specs=(row_spec, P(None, None), P(None, None), P("tp", None), P("tp"), P(("dp", "tp"))), out_specs=(P("dp"), row_spec, P("dp", None), P("dp", None)), check_vma=False)
```

```python
import functools
import math
import jax
import jax.numpy as jnp
from jax import lax
from jax.experimental import pallas as pl
from jax.experimental.pallas import tpu as pltpu
from jax.sharding import PartitionSpec as P

MESH = pl.DeviceIdType.MESH
DMA = pltpu.SemaphoreType.DMA
F32, BF16 = jnp.float32, jnp.bfloat16
LOG2E = 1.4426950408889634
BLOCKS = 8
QB = 256
SUB = 512
UNROLL = 4


def peer(index):
    return {"tp": index}


def drain(ref, sem):
    pltpu.make_async_copy(ref, ref, sem).wait()


def slot_of(d, n):
    core, chip = d % 2, d // 2
    if n == 128:
        x, y, z = chip % 4, (chip // 4) % 4, chip // 16
        return ((x + y + z) % 4) * 2 + core, z * 4 + y
    return (chip % 4) * 2 + core, chip // 4


def device_of(k, j, n):
    if n == 128:
        z, y = j // 4, j % 4
        x = (k // 2 + 8 - y - z) % 4
        return ((z * 4 + y) * 4 + x) * 2 + k % 2
    return (j * 4 + k // 2) * 2 + k % 2


def kernel(n, rows, items,
           q_ref, w1_hbm, w2_hbm, e_hbm, lq_ref, lab_ref,
           loss_ref, de_hbm, dw1_ref, dw2_ref,
           w1, w2, e, et, lqb, ids, x_mine, lab_mine, x_all, lab_all, q_all, xbt, zs,
           st_send, st_got, st_mine, st_all, de_acc, de_out, dxt, dx_part, dx_got, dx_mine, dx_all,
           t_acc, t_mine, t_all, pre, acc1, acc2,
           load_sem, out_sem, x_sem, lab_sem, q_sem, swap_sem, st_sem, stb_send, stb_recv, dx_sem, dxb_send, dxb_recv, t_sem):
    me = lax.axis_index("tp")
    ob = n // BLOCKS
    half = ob // 2
    my_k, my_j = slot_of(me, n)
    my_slot = my_k * ob + my_j
    core, chip, chips = me % 2, me // 2, n // 2
    my_row = core * chips + (my_k // 2) * ob + my_j

    loads = [pltpu.make_async_copy(a, b, load_sem.at[i]) for i, (a, b) in enumerate(((w1_hbm, w1), (w2_hbm, w2), (e_hbm, e)))]
    for c in loads:
        c.start()
    barrier = pltpu.get_barrier_semaphore()

    @pl.loop(1, n)
    def _(k):
        pl.semaphore_signal(barrier, inc=1, device_id=peer(lax.rem(me + k, n)), device_id_type=MESH)

    loads[0].wait()
    loads[1].wait()
    hid = jnp.maximum(jnp.dot(q_ref[...], w1[...], preferred_element_type=F32), 0.0).astype(BF16)
    x_mine[...] = jnp.dot(hid, w2[...], preferred_element_type=F32).astype(BF16)
    lanes = lax.broadcasted_iota(jnp.int32, (1, 128), 1)
    wide = jnp.concatenate([lab_ref[...]] * (128 // rows), axis=1) if rows < 128 else lab_ref[...]
    lab_mine[...] = jnp.where(lanes // rows == my_j % half, wide, 0)
    x_all[pl.ds(my_slot, 1)] = x_mine[...][None]
    lab_all[pl.ds(my_slot, 1)] = lab_mine[...][None]
    q_all[pl.ds(my_row, 1)] = q_ref[...][None]
    pl.semaphore_wait(barrier, n - 1)

    @pl.loop(1, n)
    def _(k):
        to = peer(lax.rem(me + k, n))
        pltpu.make_async_remote_copy(x_mine, x_all.at[my_slot], x_sem.at[0], x_sem.at[1], device_id=to, device_id_type=MESH).start()
        pltpu.make_async_remote_copy(lab_mine, lab_all.at[my_slot], lab_sem.at[0], lab_sem.at[1], device_id=to, device_id_type=MESH).start()

    loads[2].wait()

    @pl.loop(0, items // 128)
    def _(i):
        r = pl.multiple_of(i * 128, 128)
        lqb[pl.ds(r, 128), :] = jnp.broadcast_to(lq_ref[pl.ds(i, 1), :], (128, 128)).T
        et[:, pl.ds(r, 128)] = e[pl.ds(r, 128), :].T
        de_acc[pl.ds(r, 128), :] = jnp.zeros((128, 128), F32)

    ids[...] = lax.broadcasted_iota(jnp.int32, (SUB, 128), 0)
    t_acc[...] = jnp.zeros_like(t_acc)
    acc1[...] = jnp.zeros_like(acc1)
    acc2[...] = jnp.zeros_like(acc2)
    drain(x_all.at[pl.ds(0, n - 1)], x_sem.at[1])
    drain(lab_all.at[pl.ds(0, n - 1)], lab_sem.at[1])

    def combine_stats(k):
        @pl.when(jnp.logical_and(my_k == k, my_j % half == 0))
        def _():
            drain(st_got.at[pl.ds(0, n - 1)], st_sem.at[1])
            top = jnp.max(st_got[:, 0:1, :], axis=0)
            total = jnp.sum(st_got[:, 1:2, :] * jnp.exp(st_got[:, 0:1, :] - top[None]), axis=0)
            st_mine[...] = jnp.concatenate([top, jnp.log(total)], axis=0)
            st_all[pl.ds(k * 2 + my_j // half, 1)] = st_mine[...][None]

            @pl.loop(1, n)
            def _(i):
                pltpu.make_async_remote_copy(st_mine, st_all.at[k * 2 + my_j // half], stb_send, stb_recv.at[k * 2 + my_j // half],
                                             device_id=peer(lax.rem(me + i, n)), device_id_type=MESH).start()

    def combine_rows(k):
        @pl.when(my_k == k)
        def _():
            drain(dx_got.at[pl.ds(0, n - 1)], dx_sem.at[1])
            dx_mine[...] = jnp.sum(dx_got[...], axis=0).astype(BF16)
            dx_all[pl.ds(my_slot, 1)] = dx_mine[...][None]

            @pl.loop(1, n)
            def _(i):
                pltpu.make_async_remote_copy(dx_mine, dx_all.at[my_slot], dxb_send, dxb_recv.at[k],
                                             device_id=peer(lax.rem(me + i, n)), device_id_type=MESH).start()

    def logits(r):
        lq = lqb[pl.ds(r, SUB), :]
        z = jnp.dot(e[pl.ds(r, SUB), :], xbt[...], preferred_element_type=F32)
        return z - jnp.concatenate([lq, lq], axis=1)

    @pl.loop(0, BLOCKS)
    def _(k):
        xbt[...] = x_all[pl.ds(k * ob, ob)].reshape(QB, 128).T

        def step(i, carry):
            m, s = carry
            for u in range(UNROLL):
                z = logits(pl.multiple_of((i * UNROLL + u) * SUB, SUB)).reshape(SUB // 8, 8, QB)
                m_new = jnp.maximum(m, jnp.max(z, axis=0))
                s = s * jnp.exp2((m - m_new) * LOG2E) + jnp.sum(jnp.exp2((z - m_new[None]) * LOG2E), axis=0)
                m = m_new
            return m, s

        m, s = lax.fori_loop(0, items // (SUB * UNROLL), step, (jnp.full((8, QB), -3.0e38, F32), jnp.zeros((8, QB), F32)))
        top = jnp.max(m, axis=0, keepdims=True)
        total = jnp.sum(s * jnp.exp2((m - top) * LOG2E), axis=0, keepdims=True)
        for t in range(2):
            st_send[pl.ds(k * 2 + t, 1)] = jnp.concatenate([top[:, t * 128:(t + 1) * 128], total[:, t * 128:(t + 1) * 128]], axis=0)[None]
        for t in range(2):
            to = device_of(k, t * half, n)

            @pl.when(to != me)
            def _():
                pltpu.make_async_remote_copy(st_send.at[k * 2 + t], st_got.at[me], st_sem.at[0], st_sem.at[1], device_id=peer(to), device_id_type=MESH).start()

            @pl.when(to == me)
            def _():
                st_got[pl.ds(me, 1)] = st_send[pl.ds(k * 2 + t, 1)]

        combine_stats(k - 4)

    per_step = -(-(chips - 1) // (BLOCKS - 1))

    @pl.loop(0, BLOCKS)
    def _(k):
        @pl.loop(0, per_step)
        def _(i):
            c = k * per_step + i + 1

            @pl.when(c < chips)
            def _():
                pltpu.make_async_remote_copy(q_ref, q_all.at[my_row], q_sem.at[0], q_sem.at[1],
                                             device_id=peer(lax.rem(chip + c, chips) * 2 + core), device_id_type=MESH).start()

        for t in range(2):
            @pl.when(device_of(k, t * half, n) != me)
            def _():
                drain(st_all.at[0], stb_recv.at[k * 2 + t])

        xb = x_all[pl.ds(k * ob, ob)].reshape(QB, 128)
        xbt[...] = xb.T
        top = jnp.concatenate([st_all[k * 2, 0:1, :], st_all[k * 2 + 1, 0:1, :]], axis=1)
        shift = jnp.concatenate([st_all[k * 2, 1:2, :], st_all[k * 2 + 1, 1:2, :]], axis=1) * LOG2E + math.log2(n * rows)
        lab = jnp.concatenate([jnp.sum(lab_all[pl.ds(k * ob + t * half, half)], axis=0) for t in range(2)], axis=1) - me * items
        dxt[...] = jnp.zeros_like(dxt)

        @pl.loop(0, items // (SUB * UNROLL))
        def _(i):
            dx = dxt[...]
            tsum = t_acc[...]
            for u in range(UNROLL):
                r = pl.multiple_of((i * UNROLL + u) * SUB, SUB)
                z = logits(r)
                idv = ids[...]
                hit = jnp.concatenate([idv, idv], axis=1) == lab - r
                g = jnp.exp2((z - top) * LOG2E - shift) - jnp.where(hit, 1.0 / (n * rows), 0.0)
                tsum = tsum + jnp.sum(jnp.where(hit, z, 0.0).reshape(SUB // 8, 8, QB), axis=0)
                gb = g.astype(BF16)
                de_acc[pl.ds(r, SUB), :] += jnp.dot(gb, xb, preferred_element_type=F32)
                dx = dx + jnp.dot(et[:, pl.ds(r, SUB)], gb, preferred_element_type=F32)
            dxt[...] = dx
            t_acc[...] = tsum

        dx_part[pl.ds(k * ob, ob)] = dxt[...].T.reshape(ob, rows, 128)

        @pl.loop(0, ob)
        def _(j):
            to = device_of(k, j, n)

            @pl.when(to != me)
            def _():
                pltpu.make_async_remote_copy(dx_part.at[k * ob + j], dx_got.at[me], dx_sem.at[0], dx_sem.at[1], device_id=peer(to), device_id_type=MESH).start()

            @pl.when(to == me)
            def _():
                dx_got[pl.ds(me, 1)] = dx_part[pl.ds(k * ob + j, 1)]

        @pl.when(k < 4)
        def _():
            combine_stats(k + 4)

        combine_rows(k - 2)

    t_mine[...] = jnp.sum(t_acc[:, 0:128] + t_acc[:, 128:256], axis=0, keepdims=True)
    t_all[pl.ds(me, 1)] = t_mine[...][None]

    @pl.loop(1, n)
    def _(i):
        pltpu.make_async_remote_copy(t_mine, t_all.at[me], t_sem.at[0], t_sem.at[1], device_id=peer(lax.rem(me + i, n)), device_id_type=MESH).start()

    drain(q_all.at[pl.ds(0, chips - 1)], q_sem.at[1])
    swap = pltpu.make_async_remote_copy(q_all.at[pl.ds(core * chips, chips)], q_all.at[pl.ds(core * chips, chips)], swap_sem.at[0], swap_sem.at[1], device_id=peer(chip * 2 + 1 - core), device_id_type=MESH)
    swap.start()

    @pl.loop(0, items // SUB)
    def _(i):
        r = pl.multiple_of(i * SUB, SUB)
        de_out[pl.ds(r, SUB), :] = de_acc[pl.ds(r, SUB), :].astype(BF16)

    out = pltpu.make_async_copy(de_out, de_hbm, out_sem)
    out.start()
    drain(q_all.at[pl.ds(0, chips)], swap_sem.at[1])

    def rows_of(k):
        return q_all[pl.ds((k % 2) * chips + (k // 2) * ob, ob)].reshape(QB, q_all.shape[-1])

    @pl.loop(0, BLOCKS)
    def _(k):
        pre[pl.ds(k, 1)] = jnp.dot(rows_of(k), w1[...], preferred_element_type=F32)[None]

    def tower(k):
        @pl.when(my_k == k)
        def _():
            if ob > 1:
                drain(dx_all.at[pl.ds(0, ob - 1)], dxb_recv.at[k])

        @pl.when(my_k != k)
        def _():
            drain(dx_all.at[pl.ds(0, ob)], dxb_recv.at[k])

        dx = dx_all[pl.ds(k * ob, ob)].reshape(QB, 128)
        a = pre[k]
        h = jnp.maximum(a, 0.0).astype(BF16)
        acc2[...] += lax.dot_general(h, dx, (((0,), (0,)), ((), ())), preferred_element_type=F32)
        dh = lax.dot_general(dx, w2[...], (((1,), (1,)), ((), ())), preferred_element_type=F32)
        da = jnp.where(a > 0.0, dh, 0.0).astype(BF16)
        acc1[...] += lax.dot_general(rows_of(k), da, (((0,), (0,)), ((), ())), preferred_element_type=F32)

    combine_rows(BLOCKS - 2)
    pl.loop(0, BLOCKS - 3)(tower)
    combine_rows(BLOCKS - 1)
    pl.loop(BLOCKS - 3, BLOCKS)(tower)
    dw1_ref[...] = acc1[...].astype(BF16)
    dw2_ref[...] = acc2[...].astype(BF16)

    drain(t_all.at[pl.ds(0, n - 1)], t_sem.at[1])
    lse = st_all[:, 0:1, :] + st_all[:, 1:2, :]
    total = jnp.sum(lse, axis=0) - jnp.sum(t_all[...], axis=0)
    loss_ref[0] = jnp.sum(total) / (n * rows)

    out.wait()
    swap.wait_send()
    drain(x_all.at[pl.ds(0, n - 1)], x_sem.at[0])
    drain(lab_all.at[pl.ds(0, n - 1)], lab_sem.at[0])
    drain(q_all.at[pl.ds(0, chips - 1)], q_sem.at[0])
    drain(t_all.at[pl.ds(0, n - 1)], t_sem.at[0])
    drain(dx_got.at[pl.ds(0, n - 1)], dx_sem.at[0])

    @pl.when(my_j % half == 0)
    def _():
        drain(st_got.at[pl.ds(0, n - 1)], stb_send)
        drain(st_got.at[pl.ds(0, 2 * BLOCKS - 1)], st_sem.at[0])

    @pl.when(my_j % half != 0)
    def _():
        drain(st_got.at[pl.ds(0, 2 * BLOCKS)], st_sem.at[0])

    drain(dx_all.at[pl.ds(0, n - 1)], dxb_send)


def solution(mesh):
    n = mesh.shape["tp"]

    def local_step(queries, w_first, w_second, catalogue, log_q, labels):
        rows, width = queries.shape
        items = catalogue.shape[0]
        hidden = w_first.shape[1]
        ob = n // BLOCKS
        V, ANY = pl.BlockSpec(memory_space=pltpu.VMEM), pl.BlockSpec(memory_space=pl.ANY)
        S = jax.ShapeDtypeStruct
        M = pltpu.VMEM
        i32 = jnp.int32
        loss, grad_items, grad_first, grad_second = pl.pallas_call(
            functools.partial(kernel, n, rows, items),
            name="two_tower",
            out_shape=(S((1,), F32), S((items, 128), BF16), S((width, hidden), BF16), S((hidden, 128), BF16)),
            in_specs=[V, ANY, ANY, ANY, V, V],
            out_specs=(pl.BlockSpec(memory_space=pltpu.SMEM), ANY, V, V),
            scratch_shapes=[
                M((width, hidden), BF16), M((hidden, 128), BF16), M((items, 128), BF16), M((128, items), BF16), M((items, 128), F32), M((SUB, 128), i32),
                M((rows, 128), BF16), M((1, 128), i32), M((n, rows, 128), BF16), M((n, 1, 128), i32), M((n, rows, width), BF16), M((128, QB), BF16), M((8, 128), F32),
                M((2 * BLOCKS, 2, 128), F32), M((n, 2, 128), F32), M((2, 128), F32), M((2 * BLOCKS, 2, 128), F32), M((items, 128), F32), M((items, 128), BF16), M((128, QB), F32),
                M((n, rows, 128), F32), M((n, rows, 128), F32), M((rows, 128), BF16), M((n, rows, 128), BF16),
                M((8, QB), F32), M((1, 128), F32), M((n, 1, 128), F32), M((BLOCKS, QB, hidden), F32), M((width, hidden), F32), M((hidden, 128), F32),
                DMA((3,)), DMA, DMA((2,)), DMA((2,)), DMA((2,)), DMA((2,)), DMA((2,)), DMA, DMA((2 * BLOCKS,)), DMA((2,)), DMA, DMA((BLOCKS,)), DMA((2,)),
            ],
            compiler_params=pltpu.CompilerParams(collective_id=0, has_side_effects=True, vmem_limit_bytes=60 << 20),
        )(queries, w_first, w_second, catalogue, log_q.reshape(items // 128, 128), labels.reshape(1, rows))
        return loss, grad_items, grad_first, grad_second

    row_spec = P(("dp", "tp"), None)
    return jax.shard_map(local_step, mesh=mesh, in_specs=(row_spec, P(None, None), P(None, None), P("tp", None), P("tp"), P(("dp", "tp"))), out_specs=(P("dp"), row_spec, P("dp", None), P("dp", None)), check_vma=False)
```

```python
import functools
import math
import jax
import jax.numpy as jnp
from jax import lax
from jax.experimental import pallas as pl
from jax.experimental.pallas import tpu as pltpu
from jax.sharding import PartitionSpec as P

MESH = pl.DeviceIdType.MESH
DMA = pltpu.SemaphoreType.DMA
F32, BF16 = jnp.float32, jnp.bfloat16
LOG2E = 1.4426950408889634
BLOCKS = 8
LOW = -3.0e38
QB = 256
SUB = 512
UNROLL = 16


def peer(index):
    return {"tp": index}


def drain(ref, sem):
    pltpu.make_async_copy(ref, ref, sem).wait()


def slot_of(d, n):
    core, chip = d % 2, d // 2
    if n == 128:
        x, y, z = chip % 4, (chip // 4) % 4, chip // 16
        return ((x + y + z) % 4) * 2 + core, z * 4 + y
    return (chip % 4) * 2 + core, chip // 4


def device_of(k, j, n):
    if n == 128:
        z, y = j // 4, j % 4
        x = (k // 2 + 8 - y - z) % 4
        return ((z * 4 + y) * 4 + x) * 2 + k % 2
    return (j * 4 + k // 2) * 2 + k % 2


def split3(v):
    big = float(jnp.finfo(BF16).max)
    a = jnp.clip(v, -big, big).astype(BF16).astype(F32)
    b = (v - a).astype(BF16).astype(F32)
    return [a, b, v - a - b]


def stack_rows(values, height, width=128):
    at = lax.broadcasted_iota(jnp.int32, (height, width), 0)
    out = jnp.zeros((height, width), F32)
    for i, v in enumerate(values):
        out = jnp.where(at == i, v, out)
    return out


def kernel(n, rows, items,
           q_ref, w1_hbm, w2_hbm, e_hbm, lq_ref, lab_ref,
           loss_ref, de_hbm, dw1_ref, dw2_ref,
           w1, w2, e, et, ids, x_mine, lab_mine, x_all, lab_all, q_all, xa, xb, za, zb, ga, gb,
           st_send, st_got, st_mine, st_all, de_acc, de_out, dxt, dx_part, dx_got, dx_mine, dx_all,
           t_acc, t_mine, t_all, pre, acc1, acc2,
           load_sem, out_sem, x_sem, xs_sem, lab_sem, q_sem, swap_sem, st_sem, stb_send, stb_recv, dx_sem, dxb_send, dxb_recv, t_sem):
    me = lax.axis_index("tp")
    ob = n // BLOCKS
    half = ob // 2
    my_k, my_j = slot_of(me, n)
    my_slot = my_k * ob + my_j
    core, chip, chips = me % 2, me // 2, n // 2
    my_row = core * chips + (my_k // 2) * ob + my_j

    def row0(k):
        return (k % 2) * chips + (k // 2) * ob

    def swap_cores(ref, sem):
        part = ref.at[pl.ds(core * chips, chips)]
        return pltpu.make_async_remote_copy(part, part, sem.at[0], sem.at[1], device_id=peer(chip * 2 + 1 - core), device_id_type=MESH)

    loads = [pltpu.make_async_copy(a, b, load_sem.at[i]) for i, (a, b) in enumerate(((w1_hbm, w1), (w2_hbm, w2), (e_hbm, e.at[:, 0:128])))]
    for c in loads:
        c.start()
    barrier = pltpu.get_barrier_semaphore()

    @pl.loop(1, n)
    def _(k):
        pl.semaphore_signal(barrier, inc=1, device_id=peer(lax.rem(me + k, n)), device_id_type=MESH)

    loads[0].wait()
    loads[1].wait()
    hid = jnp.maximum(jnp.dot(q_ref[...], w1[...], preferred_element_type=F32), 0.0).astype(BF16)
    x_mine[...] = jnp.dot(hid, w2[...], preferred_element_type=F32).astype(BF16)
    lanes = lax.broadcasted_iota(jnp.int32, (1, 128), 1)
    wide = jnp.concatenate([lab_ref[...]] * (128 // rows), axis=1) if rows < 128 else lab_ref[...]
    lab_mine[...] = jnp.where(lanes // rows == my_j % half, wide, 0)
    x_all[pl.ds(my_row, 1)] = x_mine[...][None]
    lab_all[pl.ds(my_row, 1)] = lab_mine[...][None]
    q_all[pl.ds(my_row, 1)] = q_ref[...][None]
    loads[2].wait()

    @pl.loop(0, items // 128)
    def _(i):
        r = pl.multiple_of(i * 128, 128)
        extra = stack_rows(split3(-lq_ref[pl.ds(i, 1), :]) + [1.0] * 6, 16)
        e[pl.ds(r, 128), 128:256] = jnp.concatenate([extra, jnp.zeros((112, 128), F32)], axis=0).T.astype(BF16)
        et[:, pl.ds(r, 128)] = e[pl.ds(r, 128), 0:128].T
        de_acc[pl.ds(r, 128), :] = jnp.zeros((128, 128), F32)

    ids[...] = lax.broadcasted_iota(jnp.int32, (SUB, 128), 0)
    xa[144:256, :] = jnp.zeros((112, QB), BF16)
    t_acc[...] = jnp.zeros_like(t_acc)
    acc1[...] = jnp.zeros_like(acc1)
    acc2[...] = jnp.zeros_like(acc2)
    pl.semaphore_wait(barrier, n - 1)

    @pl.loop(1, chips)
    def _(k):
        to = peer(lax.rem(chip + k, chips) * 2 + core)
        pltpu.make_async_remote_copy(x_mine, x_all.at[my_row], x_sem.at[0], x_sem.at[1], device_id=to, device_id_type=MESH).start()

    drain(x_all.at[pl.ds(0, chips - 1)], x_sem.at[1])
    swap_x = swap_cores(x_all, xs_sem)
    swap_x.start()

    @pl.loop(1, n)
    def _(k):
        pltpu.make_async_remote_copy(lab_mine, lab_all.at[my_row], lab_sem.at[0], lab_sem.at[1], device_id=peer(lax.rem(me + k, n)), device_id_type=MESH).start()

    drain(x_all.at[pl.ds(0, chips)], xs_sem.at[1])


    def combine_stats(k):
        @pl.when(jnp.logical_and(my_k == k, my_j % half == 0))
        def _():
            drain(st_got.at[pl.ds(0, n - 1)], st_sem.at[1])
            top = jnp.max(st_got[:, 0:1, :], axis=0)
            total = jnp.sum(st_got[:, 1:2, :] * jnp.exp(st_got[:, 0:1, :] - top[None]), axis=0)
            st_mine[...] = jnp.concatenate([top, jnp.log(total)], axis=0)
            st_all[pl.ds(k * 2 + my_j // half, 1)] = st_mine[...][None]

            @pl.loop(1, n)
            def _(i):
                pltpu.make_async_remote_copy(st_mine, st_all.at[k * 2 + my_j // half], stb_send, stb_recv.at[k * 2 + my_j // half],
                                             device_id=peer(lax.rem(me + i, n)), device_id_type=MESH).start()

    def combine_rows(k):
        @pl.when(my_k == k)
        def _():
            drain(dx_got.at[pl.ds(0, n - 1)], dx_sem.at[1])
            dx_mine[...] = jnp.sum(dx_got[...], axis=0).astype(BF16)
            dx_all[pl.ds(my_slot, 1)] = dx_mine[...][None]

            @pl.loop(1, n)
            def _(i):
                pltpu.make_async_remote_copy(dx_mine, dx_all.at[my_slot], dxb_send, dxb_recv.at[k],
                                             device_id=peer(lax.rem(me + i, n)), device_id_type=MESH).start()

    def logits(q):
        return jnp.dot(e[pl.ds(pl.multiple_of(q * SUB, SUB), SUB), :], xa[...], preferred_element_type=F32)

    chunks = items // SUB

    def merge(tops, sums):
        top = functools.reduce(jnp.maximum, tops)
        return top, sum(s * jnp.exp2((m - top) * LOG2E) for m, s in zip(tops, sums))

    def exp_sum(ref, m):
        total = jnp.zeros((8, QB), F32)
        for g in range(SUB // 8):
            total = total + jnp.exp2((ref[8 * g:8 * g + 8, :] - m) * LOG2E)
        return total

    @pl.loop(0, BLOCKS)
    def _(k):
        xa[0:128, :] = x_all[pl.ds(row0(k), ob)].reshape(QB, 128).T
        xa[128:144, :] = stack_rows([1.0] * 3, 16, QB).astype(BF16)

        def step(i, carry):
            m, s, m_last = carry
            tops, sums = [m], [s]
            for u in range(UNROLL):
                new, old = (za, zb) if u % 2 == 0 else (zb, za)
                z = logits(i * UNROLL + u)
                new[...] = z
                tops.append(m_last)
                sums.append(exp_sum(old, m_last))
                m_last = functools.reduce(jnp.maximum, [z[8 * g:8 * g + 8, :] for g in range(SUB // 8)])
            return merge(tops, sums) + (m_last,)

        low = jnp.full((8, QB), LOW, F32)
        zb[...] = jnp.full((SUB, QB), LOW, F32)
        m, s, m_last = lax.fori_loop(0, chunks // UNROLL, step, (low, jnp.zeros((8, QB), F32), low))
        m, s = merge([m, m_last], [s, exp_sum(zb, m_last)])
        top = jnp.max(m, axis=0, keepdims=True)
        total = jnp.sum(s * jnp.exp2((m - top) * LOG2E), axis=0, keepdims=True)
        for t in range(2):
            st_send[pl.ds(k * 2 + t, 1)] = jnp.concatenate([top[:, t * 128:(t + 1) * 128], total[:, t * 128:(t + 1) * 128]], axis=0)[None]
        for t in range(2):
            to = device_of(k, t * half, n)

            @pl.when(to != me)
            def _():
                pltpu.make_async_remote_copy(st_send.at[k * 2 + t], st_got.at[me], st_sem.at[0], st_sem.at[1], device_id=peer(to), device_id_type=MESH).start()

            @pl.when(to == me)
            def _():
                st_got[pl.ds(me, 1)] = st_send[pl.ds(k * 2 + t, 1)]

        combine_stats(k - 4)

    drain(lab_all.at[pl.ds(0, n - 1)], lab_sem.at[1])
    per_step = -(-(chips - 1) // (BLOCKS - 2))
    swap_q = swap_cores(q_all, swap_sem)

    @pl.loop(0, BLOCKS)
    def _(k):
        @pl.loop(0, per_step)
        def _(i):
            c = k * per_step + i + 1

            @pl.when(c < chips)
            def _():
                pltpu.make_async_remote_copy(q_ref, q_all.at[my_row], q_sem.at[0], q_sem.at[1],
                                             device_id=peer(lax.rem(chip + c, chips) * 2 + core), device_id_type=MESH).start()

        @pl.when(k == BLOCKS - 1)
        def _():
            drain(q_all.at[pl.ds(0, chips - 1)], q_sem.at[1])
            swap_q.start()

        for t in range(2):
            @pl.when(device_of(k, t * half, n) != me)
            def _():
                drain(st_all.at[0], stb_recv.at[k * 2 + t])

        xb[...] = x_all[pl.ds(row0(k), ob)].reshape(QB, 128)
        xa[0:128, :] = xb[...].T
        top = jnp.concatenate([st_all[k * 2, 0:1, :], st_all[k * 2 + 1, 0:1, :]], axis=1)
        norm = jnp.concatenate([st_all[k * 2, 1:2, :], st_all[k * 2 + 1, 1:2, :]], axis=1) + math.log(n * rows)
        xa[128:144, :] = stack_rows([1.0] * 3 + split3(-top) + split3(-norm), 16, QB).astype(BF16)
        lab = jnp.concatenate([jnp.sum(lab_all[pl.ds(row0(k) + t * half, half)], axis=0) for t in range(2)], axis=1) - me * items
        dxt[...] = jnp.zeros_like(dxt)
        gb[...] = jnp.zeros_like(gb)

        zb[...] = jnp.full((SUB, QB), LOW, F32)
        ga[...] = jnp.zeros_like(ga)

        def spread(src, dst, q):
            at = lab - jnp.where(q < 0, -(1 << 29), q * SUB)
            at = jnp.broadcast_to(at, (8, QB))
            tsum = t_acc[...]
            for u in range(SUB // 16):
                parts = []
                for v in range(2):
                    rows8 = pl.ds(u * 16 + v * 8, 8)
                    z = src[rows8, :]
                    idv = ids[rows8, :]
                    hot = jnp.where(jnp.concatenate([idv, idv], axis=1) == at, 1.0 / (n * rows), 0.0)
                    tsum = tsum + z * hot
                    parts.append(jnp.exp2(z * LOG2E) - hot)
                dst[u * 16:(u + 1) * 16, :] = jnp.concatenate(parts, axis=0).astype(BF16)
            t_acc[...] = tsum

        def gather(src, q):
            r = pl.ds(pl.multiple_of(jnp.maximum(q, 0) * SUB, SUB), SUB)
            de_acc[r, :] += jnp.dot(src[...], xb[...], preferred_element_type=F32)
            dxt[...] += jnp.dot(et[:, r], src[...], preferred_element_type=F32)

        @pl.loop(0, chunks // UNROLL)
        def _(i):
            for u in range(UNROLL):
                q = i * UNROLL + u
                new, old = (za, zb) if u % 2 == 0 else (zb, za)
                here, gone = (gb, ga) if u % 2 == 0 else (ga, gb)
                new[...] = logits(q)
                spread(old, here, q - 1)
                gather(gone, q - 2)

        spread(zb, gb, chunks - 1)
        gather(ga, chunks - 2)
        gather(gb, chunks - 1)
        dx_part[pl.ds(k * ob, ob)] = dxt[...].T.reshape(ob, rows, 128)

        @pl.loop(0, ob)
        def _(j):
            to = device_of(k, j, n)

            @pl.when(to != me)
            def _():
                pltpu.make_async_remote_copy(dx_part.at[k * ob + j], dx_got.at[me], dx_sem.at[0], dx_sem.at[1], device_id=peer(to), device_id_type=MESH).start()

            @pl.when(to == me)
            def _():
                dx_got[pl.ds(me, 1)] = dx_part[pl.ds(k * ob + j, 1)]

        @pl.when(k < 4)
        def _():
            combine_stats(k + 4)

        combine_rows(k - 2)

    t_mine[...] = jnp.sum(t_acc[:, 0:128] + t_acc[:, 128:256], axis=0, keepdims=True)
    t_all[pl.ds(me, 1)] = t_mine[...][None]

    @pl.loop(1, n)
    def _(i):
        pltpu.make_async_remote_copy(t_mine, t_all.at[me], t_sem.at[0], t_sem.at[1], device_id=peer(lax.rem(me + i, n)), device_id_type=MESH).start()

    @pl.loop(0, items // 512)
    def _(i):
        r = pl.multiple_of(i * 512, 512)
        de_out[pl.ds(r, 512), :] = de_acc[pl.ds(r, 512), :].astype(BF16)

    out = pltpu.make_async_copy(de_out, de_hbm, out_sem)
    out.start()
    drain(q_all.at[pl.ds(0, chips)], swap_sem.at[1])

    def rows_of(k):
        return q_all[pl.ds(row0(k), ob)].reshape(QB, q_all.shape[-1])

    @pl.loop(0, BLOCKS)
    def _(k):
        pre[pl.ds(k, 1)] = jnp.dot(rows_of(k), w1[...], preferred_element_type=F32)[None]

    def tower(k):
        @pl.when(my_k == k)
        def _():
            if ob > 1:
                drain(dx_all.at[pl.ds(0, ob - 1)], dxb_recv.at[k])

        @pl.when(my_k != k)
        def _():
            drain(dx_all.at[pl.ds(0, ob)], dxb_recv.at[k])

        dx = dx_all[pl.ds(k * ob, ob)].reshape(QB, 128)
        a = pre[k]
        h = jnp.maximum(a, 0.0).astype(BF16)
        acc2[...] += lax.dot_general(h, dx, (((0,), (0,)), ((), ())), preferred_element_type=F32)
        dh = lax.dot_general(dx, w2[...], (((1,), (1,)), ((), ())), preferred_element_type=F32)
        da = jnp.where(a > 0.0, dh, 0.0).astype(BF16)
        acc1[...] += lax.dot_general(rows_of(k), da, (((0,), (0,)), ((), ())), preferred_element_type=F32)

    combine_rows(BLOCKS - 2)
    combine_rows(BLOCKS - 1)
    pl.loop(0, BLOCKS)(tower)
    dw1_ref[...] = acc1[...].astype(BF16)
    dw2_ref[...] = acc2[...].astype(BF16)

    drain(t_all.at[pl.ds(0, n - 1)], t_sem.at[1])
    loss_ref[0] = -jnp.sum(t_all[...]) - math.log(n * rows)

    out.wait()
    swap_q.wait_send()
    swap_x.wait_send()
    drain(x_all.at[pl.ds(0, chips - 1)], x_sem.at[0])
    drain(lab_all.at[pl.ds(0, n - 1)], lab_sem.at[0])
    drain(q_all.at[pl.ds(0, chips - 1)], q_sem.at[0])
    drain(t_all.at[pl.ds(0, n - 1)], t_sem.at[0])
    drain(dx_got.at[pl.ds(0, n - 1)], dx_sem.at[0])

    @pl.when(my_j % half == 0)
    def _():
        drain(st_got.at[pl.ds(0, n - 1)], stb_send)
        drain(st_got.at[pl.ds(0, 2 * BLOCKS - 1)], st_sem.at[0])

    @pl.when(my_j % half != 0)
    def _():
        drain(st_got.at[pl.ds(0, 2 * BLOCKS)], st_sem.at[0])

    drain(dx_all.at[pl.ds(0, n - 1)], dxb_send)


def solution(mesh):
    n = mesh.shape["tp"]

    def local_step(queries, w_first, w_second, catalogue, log_q, labels):
        rows, width = queries.shape
        items = catalogue.shape[0]
        hidden = w_first.shape[1]
        ob = n // BLOCKS
        V, ANY = pl.BlockSpec(memory_space=pltpu.VMEM), pl.BlockSpec(memory_space=pl.ANY)
        S = jax.ShapeDtypeStruct
        M = pltpu.VMEM
        i32 = jnp.int32
        loss, grad_items, grad_first, grad_second = pl.pallas_call(
            functools.partial(kernel, n, rows, items),
            name="two_tower",
            out_shape=(S((1,), F32), S((items, 128), BF16), S((width, hidden), BF16), S((hidden, 128), BF16)),
            in_specs=[V, ANY, ANY, ANY, V, V],
            out_specs=(pl.BlockSpec(memory_space=pltpu.SMEM), ANY, V, V),
            scratch_shapes=[
                M((width, hidden), BF16), M((hidden, 128), BF16), M((items, 256), BF16), M((128, items), BF16), M((SUB, 128), i32),
                M((rows, 128), BF16), M((1, 128), i32), M((n, rows, 128), BF16), M((n, 1, 128), i32), M((n, rows, width), BF16), M((256, QB), BF16), M((QB, 128), BF16), M((SUB, QB), F32), M((SUB, QB), F32), M((SUB, QB), BF16), M((SUB, QB), BF16),
                M((2 * BLOCKS, 2, 128), F32), M((n, 2, 128), F32), M((2, 128), F32), M((2 * BLOCKS, 2, 128), F32), M((items, 128), F32), M((items, 128), BF16), M((128, QB), F32),
                M((n, rows, 128), F32), M((n, rows, 128), F32), M((rows, 128), BF16), M((n, rows, 128), BF16),
                M((8, QB), F32), M((1, 128), F32), M((n, 1, 128), F32), M((BLOCKS, QB, hidden), F32), M((width, hidden), F32), M((hidden, 128), F32),
                DMA((3,)), DMA, DMA((2,)), DMA((2,)), DMA((2,)), DMA((2,)), DMA((2,)), DMA((2,)), DMA, DMA((2 * BLOCKS,)), DMA((2,)), DMA, DMA((BLOCKS,)), DMA((2,)),
            ],
            compiler_params=pltpu.CompilerParams(collective_id=0, has_side_effects=True, vmem_limit_bytes=60 << 20),
        )(queries, w_first, w_second, catalogue, log_q.reshape(items // 128, 128), labels.reshape(1, rows))
        return loss, grad_items, grad_first, grad_second

    row_spec = P(("dp", "tp"), None)
    return jax.shard_map(local_step, mesh=mesh, in_specs=(row_spec, P(None, None), P(None, None), P("tp", None), P("tp"), P(("dp", "tp"))), out_specs=(P("dp"), row_spec, P("dp", None), P("dp", None)), check_vma=False)
```

```python
import functools
import math
import jax
import jax.numpy as jnp
from jax import lax
from jax.experimental import pallas as pl
from jax.experimental.pallas import tpu as pltpu
from jax.sharding import PartitionSpec as P

MESH = pl.DeviceIdType.MESH
DMA = pltpu.SemaphoreType.DMA
F32, BF16 = jnp.float32, jnp.bfloat16
LOG2E = 1.4426950408889634
BLOCKS = 8
LOW = -3.0e38
QB = 256
SUB = 512
UNROLL = 16


def peer(index):
    return {"tp": index}


def drain(ref, sem):
    pltpu.make_async_copy(ref, ref, sem).wait()


def slot_of(d, n):
    core, chip = d % 2, d // 2
    if n == 128:
        x, y, z = chip % 4, (chip // 4) % 4, chip // 16
        return ((x + y + z) % 4) * 2 + core, z * 4 + y
    return (chip % 4) * 2 + core, chip // 4


def device_of(k, j, n):
    if n == 128:
        z, y = j // 4, j % 4
        x = (k // 2 + 8 - y - z) % 4
        return ((z * 4 + y) * 4 + x) * 2 + k % 2
    return (j * 4 + k // 2) * 2 + k % 2


def split3(v):
    big = float(jnp.finfo(BF16).max)
    a = jnp.clip(v, -big, big).astype(BF16).astype(F32)
    b = (v - a).astype(BF16).astype(F32)
    return [a, b, v - a - b]


def stack_rows(values, height, width=128):
    at = lax.broadcasted_iota(jnp.int32, (height, width), 0)
    out = jnp.zeros((height, width), F32)
    for i, v in enumerate(values):
        out = jnp.where(at == i, v, out)
    return out


def kernel(n, rows, items,
           q_ref, w1_hbm, w2_hbm, e_hbm, lq_ref, lab_ref,
           loss_ref, de_hbm, dw1_ref, dw2_ref,
           w1, w2, e, et, ids, x_mine, lab_mine, x_all, lab_all, q_all, xa, xb, za, zb, ga, gb,
           st_send, st_got, st_mine, st_all, de_acc, de_out, dxt, dx_part, pair, dx_sum, dx_got, dx_mine, dx_all,
           t_acc, t_mine, t_all, pre, acc1, acc2,
           load_sem, out_sem, x_sem, xs_sem, lab_sem, q_sem, swap_sem, st_sem, stb_send, stb_recv, pair_send, pair_recv, dx_sem, dxb_send, dxb_recv, t_sem):
    me = lax.axis_index("tp")
    ob = n // BLOCKS
    half = ob // 2
    my_k, my_j = slot_of(me, n)
    my_slot = my_k * ob + my_j
    core, chip, chips = me % 2, me // 2, n // 2
    my_row = core * chips + (my_k // 2) * ob + my_j

    def row0(k):
        return (k % 2) * chips + (k // 2) * ob

    def swap_cores(ref, sem):
        part = ref.at[pl.ds(core * chips, chips)]
        return pltpu.make_async_remote_copy(part, part, sem.at[0], sem.at[1], device_id=peer(chip * 2 + 1 - core), device_id_type=MESH)

    loads = [pltpu.make_async_copy(a, b, load_sem.at[i]) for i, (a, b) in enumerate(((w1_hbm, w1), (w2_hbm, w2), (e_hbm, e.at[:, 0:128])))]
    for c in loads:
        c.start()
    barrier = pltpu.get_barrier_semaphore()

    @pl.loop(1, n)
    def _(k):
        pl.semaphore_signal(barrier, inc=1, device_id=peer(lax.rem(me + k, n)), device_id_type=MESH)

    loads[0].wait()
    loads[1].wait()
    hid = jnp.maximum(jnp.dot(q_ref[...], w1[...], preferred_element_type=F32), 0.0).astype(BF16)
    x_mine[...] = jnp.dot(hid, w2[...], preferred_element_type=F32).astype(BF16)
    lanes = lax.broadcasted_iota(jnp.int32, (1, 128), 1)
    wide = jnp.concatenate([lab_ref[...]] * (128 // rows), axis=1) if rows < 128 else lab_ref[...]
    lab_mine[...] = jnp.where(lanes // rows == my_j % half, wide, 0)
    x_all[pl.ds(my_row, 1)] = x_mine[...][None]
    lab_all[pl.ds(my_row, 1)] = lab_mine[...][None]
    q_all[pl.ds(my_row, 1)] = q_ref[...][None]
    loads[2].wait()

    @pl.loop(0, items // 1024)
    def _(i):
        parts = split3(-lq_ref[pl.ds(pl.multiple_of(i * 8, 8), 8), :])
        for u in range(8):
            r = pl.multiple_of(i * 1024 + u * 128, 128)
            extra = stack_rows([p[u:u + 1, :] for p in parts] + [1.0] * 6, 16)
            e[pl.ds(r, 128), 128:256] = jnp.concatenate([extra, jnp.zeros((112, 128), F32)], axis=0).T.astype(BF16)
            et[:, pl.ds(r, 128)] = e[pl.ds(r, 128), 0:128].T
            de_acc[pl.ds(r, 128), :] = jnp.zeros((128, 128), F32)

    ids[...] = lax.broadcasted_iota(jnp.int32, (SUB, 128), 0)
    xa[144:256, :] = jnp.zeros((112, QB), BF16)
    t_acc[...] = jnp.zeros_like(t_acc)
    acc1[...] = jnp.zeros_like(acc1)
    acc2[...] = jnp.zeros_like(acc2)
    pl.semaphore_wait(barrier, n - 1)

    @pl.loop(1, chips)
    def _(k):
        to = peer(lax.rem(chip + k, chips) * 2 + core)
        pltpu.make_async_remote_copy(x_mine, x_all.at[my_row], x_sem.at[0], x_sem.at[1], device_id=to, device_id_type=MESH).start()

    drain(x_all.at[pl.ds(0, chips - 1)], x_sem.at[1])
    swap_x = swap_cores(x_all, xs_sem)
    swap_x.start()

    @pl.loop(1, n)
    def _(k):
        pltpu.make_async_remote_copy(lab_mine, lab_all.at[my_row], lab_sem.at[0], lab_sem.at[1], device_id=peer(lax.rem(me + k, n)), device_id_type=MESH).start()

    drain(x_all.at[pl.ds(0, chips)], xs_sem.at[1])


    def combine_stats(k):
        @pl.when(jnp.logical_and(my_k == k, my_j % half == 0))
        def _():
            drain(st_got.at[pl.ds(0, n - 1)], st_sem.at[1])
            top = jnp.max(st_got[:, 0:1, :], axis=0)
            total = jnp.sum(st_got[:, 1:2, :] * jnp.exp(st_got[:, 0:1, :] - top[None]), axis=0)
            st_mine[...] = jnp.concatenate([top, jnp.log(total)], axis=0)
            st_all[pl.ds(k * 2 + my_j // half, 1)] = st_mine[...][None]

            @pl.loop(1, n)
            def _(i):
                pltpu.make_async_remote_copy(st_mine, st_all.at[k * 2 + my_j // half], stb_send, stb_recv.at[k * 2 + my_j // half],
                                             device_id=peer(lax.rem(me + i, n)), device_id_type=MESH).start()

    def flush(k):
        drain(pair.at[pl.ds(0, half)], pair_recv.at[k])
        dx_sum[pl.ds(k * half, half)] = dx_part[pl.ds(k * ob + core * half, half)] + pair[pl.ds(k * half, half)]

        @pl.loop(0, half)
        def _(j):
            to = device_of(k, core * half + j, n)

            @pl.when(to != me)
            def _():
                pltpu.make_async_remote_copy(dx_sum.at[k * half + j], dx_got.at[chip], dx_sem.at[0], dx_sem.at[1], device_id=peer(to), device_id_type=MESH).start()

            @pl.when(to == me)
            def _():
                dx_got[pl.ds(chip, 1)] = dx_sum[pl.ds(k * half + j, 1)]

    own_half = my_j // half == core

    def combine_rows(k):
        @pl.when(my_k == k)
        def _():
            @pl.when(own_half)
            def _():
                drain(dx_got.at[pl.ds(0, chips - 1)], dx_sem.at[1])

            @pl.when(jnp.logical_not(own_half))
            def _():
                drain(dx_got.at[pl.ds(0, chips)], dx_sem.at[1])

            dx_mine[...] = jnp.sum(dx_got[...], axis=0).astype(BF16)
            dx_all[pl.ds(my_slot, 1)] = dx_mine[...][None]

            @pl.loop(1, n)
            def _(i):
                pltpu.make_async_remote_copy(dx_mine, dx_all.at[my_slot], dxb_send, dxb_recv.at[k],
                                             device_id=peer(lax.rem(me + i, n)), device_id_type=MESH).start()

    def logits(q):
        return jnp.dot(e[pl.ds(pl.multiple_of(q * SUB, SUB), SUB), :], xa[...], preferred_element_type=F32)

    chunks = items // SUB

    def merge(tops, sums):
        top = functools.reduce(jnp.maximum, tops)
        return top, sum(s * jnp.exp2((m - top) * LOG2E) for m, s in zip(tops, sums))

    def exp_sum(ref, m):
        total = jnp.zeros((8, QB), F32)
        for g in range(SUB // 8):
            total = total + jnp.exp2((ref[8 * g:8 * g + 8, :] - m) * LOG2E)
        return total

    per_step = -(-(chips - 1) // (2 * BLOCKS - 2))

    def send_rows(step):
        @pl.loop(0, per_step)
        def _(i):
            c = step * per_step + i + 1

            @pl.when(c < chips)
            def _():
                pltpu.make_async_remote_copy(q_ref, q_all.at[my_row], q_sem.at[0], q_sem.at[1],
                                             device_id=peer(lax.rem(chip + c, chips) * 2 + core), device_id_type=MESH).start()

    @pl.loop(0, BLOCKS)
    def _(k):
        xa[0:128, :] = x_all[pl.ds(row0(k), ob)].reshape(QB, 128).T
        xa[128:144, :] = stack_rows([1.0] * 3, 16, QB).astype(BF16)

        def step(i, carry):
            m, s, m_last = carry
            tops, sums = [m], [s]
            for u in range(UNROLL):
                new, old = (za, zb) if u % 2 == 0 else (zb, za)
                z = logits(i * UNROLL + u)
                new[...] = z
                tops.append(m_last)
                sums.append(exp_sum(old, m_last))
                m_last = functools.reduce(jnp.maximum, [z[8 * g:8 * g + 8, :] for g in range(SUB // 8)])
            return merge(tops, sums) + (m_last,)

        low = jnp.full((8, QB), LOW, F32)
        zb[...] = jnp.full((SUB, QB), LOW, F32)
        m, s, m_last = lax.fori_loop(0, chunks // UNROLL, step, (low, jnp.zeros((8, QB), F32), low))
        m, s = merge([m, m_last], [s, exp_sum(zb, m_last)])
        top = jnp.max(m, axis=0, keepdims=True)
        total = jnp.sum(s * jnp.exp2((m - top) * LOG2E), axis=0, keepdims=True)
        for t in range(2):
            st_send[pl.ds(k * 2 + t, 1)] = jnp.concatenate([top[:, t * 128:(t + 1) * 128], total[:, t * 128:(t + 1) * 128]], axis=0)[None]
        for t in range(2):
            to = device_of(k, t * half, n)

            @pl.when(to != me)
            def _():
                pltpu.make_async_remote_copy(st_send.at[k * 2 + t], st_got.at[me], st_sem.at[0], st_sem.at[1], device_id=peer(to), device_id_type=MESH).start()

            @pl.when(to == me)
            def _():
                st_got[pl.ds(me, 1)] = st_send[pl.ds(k * 2 + t, 1)]

        send_rows(k)
        combine_stats(k - 4)

    drain(lab_all.at[pl.ds(0, n - 1)], lab_sem.at[1])
    swap_q = swap_cores(q_all, swap_sem)

    @pl.loop(0, BLOCKS)
    def _(k):
        send_rows(BLOCKS + k)

        @pl.when(k == BLOCKS - 1)
        def _():
            drain(q_all.at[pl.ds(0, chips - 1)], q_sem.at[1])
            swap_q.start()

        for t in range(2):
            @pl.when(device_of(k, t * half, n) != me)
            def _():
                drain(st_all.at[0], stb_recv.at[k * 2 + t])

        xb[...] = x_all[pl.ds(row0(k), ob)].reshape(QB, 128)
        xa[0:128, :] = xb[...].T
        top = jnp.concatenate([st_all[k * 2, 0:1, :], st_all[k * 2 + 1, 0:1, :]], axis=1)
        norm = jnp.concatenate([st_all[k * 2, 1:2, :], st_all[k * 2 + 1, 1:2, :]], axis=1) + math.log(n * rows)
        xa[128:144, :] = stack_rows([1.0] * 3 + split3(-top) + split3(-norm), 16, QB).astype(BF16)
        lab = jnp.concatenate([jnp.sum(lab_all[pl.ds(row0(k) + t * half, half)], axis=0) for t in range(2)], axis=1) - me * items
        dxt[...] = jnp.zeros_like(dxt)
        gb[...] = jnp.zeros_like(gb)

        zb[...] = jnp.full((SUB, QB), LOW, F32)
        ga[...] = jnp.zeros_like(ga)

        def spread(src, dst, q):
            at = lab - jnp.where(q < 0, -(1 << 29), q * SUB)
            at = jnp.broadcast_to(at, (8, QB))
            tsum = t_acc[...]
            for u in range(SUB // 16):
                parts = []
                for v in range(2):
                    rows8 = pl.ds(u * 16 + v * 8, 8)
                    z = src[rows8, :]
                    idv = ids[rows8, :]
                    hot = jnp.where(jnp.concatenate([idv, idv], axis=1) == at, 1.0 / (n * rows), 0.0)
                    tsum = tsum + z * hot
                    parts.append(jnp.exp2(z * LOG2E) - hot)
                dst[u * 16:(u + 1) * 16, :] = jnp.concatenate(parts, axis=0).astype(BF16)
            t_acc[...] = tsum

        def gather(src, q):
            r = pl.ds(pl.multiple_of(jnp.maximum(q, 0) * SUB, SUB), SUB)
            de_acc[r, :] += jnp.dot(src[...], xb[...], preferred_element_type=F32)
            dxt[...] += jnp.dot(et[:, r], src[...], preferred_element_type=F32)

        @pl.loop(0, chunks // UNROLL)
        def _(i):
            for u in range(UNROLL):
                q = i * UNROLL + u
                new, old = (za, zb) if u % 2 == 0 else (zb, za)
                here, gone = (gb, ga) if u % 2 == 0 else (ga, gb)
                new[...] = logits(q)
                spread(old, here, q - 1)
                gather(gone, q - 2)

        @pl.when(k > 0)
        def _():
            flush(k - 1)

        spread(zb, gb, chunks - 1)
        gather(ga, chunks - 2)
        gather(gb, chunks - 1)
        dx_part[pl.ds(k * ob, ob)] = dxt[...].T.reshape(ob, rows, 128)

        pltpu.make_async_remote_copy(dx_part.at[pl.ds(k * ob + (1 - core) * half, half)], pair.at[pl.ds(k * half, half)], pair_send, pair_recv.at[k],
                                     device_id=peer(chip * 2 + 1 - core), device_id_type=MESH).start()

        @pl.when(k < 4)
        def _():
            combine_stats(k + 4)

        combine_rows(k - 3)

    t_mine[...] = jnp.sum(t_acc[:, 0:128] + t_acc[:, 128:256], axis=0, keepdims=True)
    t_all[pl.ds(me, 1)] = t_mine[...][None]

    @pl.loop(1, n)
    def _(i):
        pltpu.make_async_remote_copy(t_mine, t_all.at[me], t_sem.at[0], t_sem.at[1], device_id=peer(lax.rem(me + i, n)), device_id_type=MESH).start()

    flush(BLOCKS - 1)

    @pl.loop(0, items // 512)
    def _(i):
        r = pl.multiple_of(i * 512, 512)
        de_out[pl.ds(r, 512), :] = de_acc[pl.ds(r, 512), :].astype(BF16)

    out = pltpu.make_async_copy(de_out, de_hbm, out_sem)
    out.start()
    drain(q_all.at[pl.ds(0, chips)], swap_sem.at[1])

    def rows_of(k):
        return q_all[pl.ds(row0(k), ob)].reshape(QB, q_all.shape[-1])

    @pl.loop(0, BLOCKS)
    def _(k):
        pre[pl.ds(k, 1)] = jnp.dot(rows_of(k), w1[...], preferred_element_type=F32)[None]

    def tower(k):
        @pl.when(my_k == k)
        def _():
            if ob > 1:
                drain(dx_all.at[pl.ds(0, ob - 1)], dxb_recv.at[k])

        @pl.when(my_k != k)
        def _():
            drain(dx_all.at[pl.ds(0, ob)], dxb_recv.at[k])

        dx = dx_all[pl.ds(k * ob, ob)].reshape(QB, 128)
        a = pre[k]
        h = jnp.maximum(a, 0.0).astype(BF16)
        acc2[...] += lax.dot_general(h, dx, (((0,), (0,)), ((), ())), preferred_element_type=F32)
        dh = lax.dot_general(dx, w2[...], (((1,), (1,)), ((), ())), preferred_element_type=F32)
        da = jnp.where(a > 0.0, dh, 0.0).astype(BF16)
        acc1[...] += lax.dot_general(rows_of(k), da, (((0,), (0,)), ((), ())), preferred_element_type=F32)

    combine_rows(BLOCKS - 3)
    combine_rows(BLOCKS - 2)
    combine_rows(BLOCKS - 1)
    pl.loop(0, BLOCKS)(tower)
    dw1_ref[...] = acc1[...].astype(BF16)
    dw2_ref[...] = acc2[...].astype(BF16)

    drain(t_all.at[pl.ds(0, n - 1)], t_sem.at[1])
    loss_ref[0] = -jnp.sum(t_all[...]) - math.log(n * rows)

    out.wait()
    swap_q.wait_send()
    swap_x.wait_send()
    drain(x_all.at[pl.ds(0, chips - 1)], x_sem.at[0])
    drain(lab_all.at[pl.ds(0, n - 1)], lab_sem.at[0])
    drain(q_all.at[pl.ds(0, chips - 1)], q_sem.at[0])
    drain(t_all.at[pl.ds(0, n - 1)], t_sem.at[0])
    drain(pair.at[pl.ds(0, BLOCKS * half)], pair_send)

    @pl.when(own_half)
    def _():
        drain(dx_got.at[pl.ds(0, chips - 1)], dx_sem.at[0])

    @pl.when(jnp.logical_not(own_half))
    def _():
        drain(dx_got.at[pl.ds(0, chips)], dx_sem.at[0])

    @pl.when(my_j % half == 0)
    def _():
        drain(st_got.at[pl.ds(0, n - 1)], stb_send)
        drain(st_got.at[pl.ds(0, 2 * BLOCKS - 1)], st_sem.at[0])

    @pl.when(my_j % half != 0)
    def _():
        drain(st_got.at[pl.ds(0, 2 * BLOCKS)], st_sem.at[0])

    drain(dx_all.at[pl.ds(0, n - 1)], dxb_send)


def solution(mesh):
    n = mesh.shape["tp"]

    def local_step(queries, w_first, w_second, catalogue, log_q, labels):
        rows, width = queries.shape
        items = catalogue.shape[0]
        hidden = w_first.shape[1]
        ob = n // BLOCKS
        V, ANY = pl.BlockSpec(memory_space=pltpu.VMEM), pl.BlockSpec(memory_space=pl.ANY)
        S = jax.ShapeDtypeStruct
        M = pltpu.VMEM
        i32 = jnp.int32
        loss, grad_items, grad_first, grad_second = pl.pallas_call(
            functools.partial(kernel, n, rows, items),
            name="two_tower",
            out_shape=(S((1,), F32), S((items, 128), BF16), S((width, hidden), BF16), S((hidden, 128), BF16)),
            in_specs=[V, ANY, ANY, ANY, V, V],
            out_specs=(pl.BlockSpec(memory_space=pltpu.SMEM), ANY, V, V),
            scratch_shapes=[
                M((width, hidden), BF16), M((hidden, 128), BF16), M((items, 256), BF16), M((128, items), BF16), M((SUB, 128), i32),
                M((rows, 128), BF16), M((1, 128), i32), M((n, rows, 128), BF16), M((n, 1, 128), i32), M((n, rows, width), BF16), M((256, QB), BF16), M((QB, 128), BF16), M((SUB, QB), F32), M((SUB, QB), F32), M((SUB, QB), BF16), M((SUB, QB), BF16),
                M((2 * BLOCKS, 2, 128), F32), M((n, 2, 128), F32), M((2, 128), F32), M((2 * BLOCKS, 2, 128), F32), M((items, 128), F32), M((items, 128), BF16), M((128, QB), F32),
                M((n, rows, 128), F32), M((n // 2, rows, 128), F32), M((n // 2, rows, 128), F32), M((n // 2, rows, 128), F32), M((rows, 128), BF16), M((n, rows, 128), BF16),
                M((8, QB), F32), M((1, 128), F32), M((n, 1, 128), F32), M((BLOCKS, QB, hidden), F32), M((width, hidden), F32), M((hidden, 128), F32),
                DMA((3,)), DMA, DMA((2,)), DMA((2,)), DMA((2,)), DMA((2,)), DMA((2,)), DMA((2,)), DMA, DMA((2 * BLOCKS,)), DMA, DMA((BLOCKS,)), DMA((2,)), DMA, DMA((BLOCKS,)), DMA((2,)),
            ],
            compiler_params=pltpu.CompilerParams(collective_id=0, has_side_effects=True, vmem_limit_bytes=60 << 20),
        )(queries, w_first, w_second, catalogue, log_q.reshape(items // 128, 128), labels.reshape(1, rows))
        return loss, grad_items, grad_first, grad_second

    row_spec = P(("dp", "tp"), None)
    return jax.shard_map(local_step, mesh=mesh, in_specs=(row_spec, P(None, None), P(None, None), P("tp", None), P("tp"), P(("dp", "tp"))), out_specs=(P("dp"), row_spec, P("dp", None), P("dp", None)), check_vma=False)
```

```python
import functools
import math
import jax
import jax.numpy as jnp
from jax import lax
from jax.experimental import pallas as pl
from jax.experimental.pallas import tpu as pltpu
from jax.sharding import PartitionSpec as P

MESH = pl.DeviceIdType.MESH
DMA = pltpu.SemaphoreType.DMA
F32, BF16 = jnp.float32, jnp.bfloat16
LOG2E = 1.4426950408889634
BLOCKS = 8
LOW = -3.0e38
QB = 256
SUB = 512
UNROLL = 16


def peer(index):
    return {"tp": index}


def drain(ref, sem):
    pltpu.make_async_copy(ref, ref, sem).wait()


def slot_of(d, n):
    core, chip = d % 2, d // 2
    if n == 128:
        x, y, z = chip % 4, (chip // 4) % 4, chip // 16
        return ((x + y + z) % 4) * 2 + core, z * 4 + y
    return (chip % 4) * 2 + core, chip // 4


def device_of(k, j, n):
    if n == 128:
        z, y = j // 4, j % 4
        x = (k // 2 + 8 - y - z) % 4
        return ((z * 4 + y) * 4 + x) * 2 + k % 2
    return (j * 4 + k // 2) * 2 + k % 2


def split3(v):
    big = float(jnp.finfo(BF16).max)
    a = jnp.clip(v, -big, big).astype(BF16).astype(F32)
    b = (v - a).astype(BF16).astype(F32)
    return [a, b, v - a - b]


def stack_rows(values, height, width=128):
    at = lax.broadcasted_iota(jnp.int32, (height, width), 0)
    out = jnp.zeros((height, width), F32)
    for i, v in enumerate(values):
        out = jnp.where(at == i, v, out)
    return out


def stat_owner(k, t, n):
    return device_of(5, 2 * k + t, n) if n == 128 else device_of(k, t * (n // BLOCKS // 2), n)


def kernel(n, rows, items,
           q_ref, w1_hbm, w2_hbm, e_hbm, lq_ref, lab_ref,
           loss_ref, de_hbm, dw1_ref, dw2_ref,
           w1, w2, e, et, ids, x_mine, lab_mine, x_all, lab_all, q_all, xa, xb, za, zb, ga, gb,
           st_send, st_got, st_mine, st_all, de_acc, de_out, dxt, dx_part, pair, dx_sum, dx_got, dx_mine, dx_all,
           t_acc, t_mine, t_all, pre, acc1, acc2,
           load_sem, out_sem, x_sem, xs_sem, lab_sem, q_sem, swap_sem, st_sem, stb_send, stb_recv, pair_send, pair_recv, dx_sem, dxb_send, dxb_recv, t_sem):
    me = lax.axis_index("tp")
    ob = n // BLOCKS
    half = ob // 2
    my_k, my_j = slot_of(me, n)
    my_slot = my_k * ob + my_j
    core, chip, chips = me % 2, me // 2, n // 2
    my_row = core * chips + (my_k // 2) * ob + my_j

    if n == 128:
        is_stat, stat_k, stat_t = my_k == 5, my_j // 2, my_j % 2
    else:
        is_stat, stat_k, stat_t = my_j % half == 0, my_k, my_j // half

    def row0(k):
        return (k % 2) * chips + (k // 2) * ob

    def swap_cores(ref, sem):
        part = ref.at[pl.ds(core * chips, chips)]
        return pltpu.make_async_remote_copy(part, part, sem.at[0], sem.at[1], device_id=peer(chip * 2 + 1 - core), device_id_type=MESH)

    loads = [pltpu.make_async_copy(a, b, load_sem.at[i]) for i, (a, b) in enumerate(((w1_hbm, w1), (w2_hbm, w2), (e_hbm, e.at[:, 0:128])))]
    for c in loads:
        c.start()
    barrier = pltpu.get_barrier_semaphore()

    @pl.loop(1, n)
    def _(k):
        pl.semaphore_signal(barrier, inc=1, device_id=peer(lax.rem(me + k, n)), device_id_type=MESH)

    loads[0].wait()
    loads[1].wait()
    hid = jnp.maximum(jnp.dot(q_ref[...], w1[...], preferred_element_type=F32), 0.0).astype(BF16)
    x_mine[...] = jnp.dot(hid, w2[...], preferred_element_type=F32).astype(BF16)
    lanes = lax.broadcasted_iota(jnp.int32, (1, 128), 1)
    wide = jnp.concatenate([lab_ref[...]] * (128 // rows), axis=1) if rows < 128 else lab_ref[...]
    lab_mine[...] = jnp.where(lanes // rows == my_j % half, wide, 0)
    x_all[pl.ds(my_row, 1)] = x_mine[...][None]
    lab_all[pl.ds(my_row, 1)] = lab_mine[...][None]
    q_all[pl.ds(my_row, 1)] = q_ref[...][None]
    loads[2].wait()

    @pl.loop(0, items // 1024)
    def _(i):
        parts = split3(-lq_ref[pl.ds(pl.multiple_of(i * 8, 8), 8), :])
        for u in range(8):
            r = pl.multiple_of(i * 1024 + u * 128, 128)
            extra = stack_rows([p[u:u + 1, :] for p in parts] + [1.0] * 6, 16)
            e[pl.ds(r, 128), 128:256] = jnp.concatenate([extra, jnp.zeros((112, 128), F32)], axis=0).T.astype(BF16)
            et[:, pl.ds(r, 128)] = e[pl.ds(r, 128), 0:128].T
            de_acc[pl.ds(r, 128), :] = jnp.zeros((128, 128), F32)

    ids[...] = lax.broadcasted_iota(jnp.int32, (SUB, 128), 0)
    xa[144:256, :] = jnp.zeros((112, QB), BF16)
    t_acc[...] = jnp.zeros_like(t_acc)
    acc1[...] = jnp.zeros_like(acc1)
    acc2[...] = jnp.zeros_like(acc2)
    pl.semaphore_wait(barrier, n - 1)

    @pl.loop(1, chips)
    def _(k):
        to = peer(lax.rem(chip + k, chips) * 2 + core)
        pltpu.make_async_remote_copy(x_mine, x_all.at[my_row], x_sem.at[0], x_sem.at[1], device_id=to, device_id_type=MESH).start()

    drain(x_all.at[pl.ds(0, chips - 1)], x_sem.at[1])
    swap_x = swap_cores(x_all, xs_sem)
    swap_x.start()

    @pl.loop(1, n)
    def _(k):
        pltpu.make_async_remote_copy(lab_mine, lab_all.at[my_row], lab_sem.at[0], lab_sem.at[1], device_id=peer(lax.rem(me + k, n)), device_id_type=MESH).start()

    drain(x_all.at[pl.ds(0, chips)], xs_sem.at[1])


    def combine_stats(k):
        @pl.when(jnp.logical_and(is_stat, stat_k == k))
        def _():
            drain(st_got.at[pl.ds(0, n - 1)], st_sem.at[1])
            top = jnp.max(st_got[:, 0:1, :], axis=0)
            total = jnp.sum(st_got[:, 1:2, :] * jnp.exp(st_got[:, 0:1, :] - top[None]), axis=0)
            st_mine[...] = jnp.concatenate([top, jnp.log(total)], axis=0)
            st_all[pl.ds(k * 2 + stat_t, 1)] = st_mine[...][None]

            @pl.loop(1, n)
            def _(i):
                pltpu.make_async_remote_copy(st_mine, st_all.at[k * 2 + stat_t], stb_send, stb_recv.at[k * 2 + stat_t],
                                             device_id=peer(lax.rem(me + i, n)), device_id_type=MESH).start()

    def flush(k):
        drain(pair.at[pl.ds(0, half)], pair_recv.at[k])
        dx_sum[pl.ds(k * half, half)] = dx_part[pl.ds(k * ob + core * half, half)] + pair[pl.ds(k * half, half)]

        @pl.loop(0, half)
        def _(j):
            to = device_of(k, core * half + j, n)

            @pl.when(to != me)
            def _():
                pltpu.make_async_remote_copy(dx_sum.at[k * half + j], dx_got.at[chip], dx_sem.at[0], dx_sem.at[1], device_id=peer(to), device_id_type=MESH).start()

            @pl.when(to == me)
            def _():
                dx_got[pl.ds(chip, 1)] = dx_sum[pl.ds(k * half + j, 1)]

    own_half = my_j // half == core

    def combine_rows(k):
        @pl.when(my_k == k)
        def _():
            @pl.when(own_half)
            def _():
                drain(dx_got.at[pl.ds(0, chips - 1)], dx_sem.at[1])

            @pl.when(jnp.logical_not(own_half))
            def _():
                drain(dx_got.at[pl.ds(0, chips)], dx_sem.at[1])

            dx_mine[...] = jnp.sum(dx_got[...], axis=0).astype(BF16)
            dx_all[pl.ds(my_slot, 1)] = dx_mine[...][None]

            @pl.loop(1, n)
            def _(i):
                pltpu.make_async_remote_copy(dx_mine, dx_all.at[my_slot], dxb_send, dxb_recv.at[k],
                                             device_id=peer(lax.rem(me + i, n)), device_id_type=MESH).start()

    def logits(q):
        return jnp.dot(e[pl.ds(pl.multiple_of(q * SUB, SUB), SUB), :], xa[...], preferred_element_type=F32)

    chunks = items // SUB

    def merge(tops, sums):
        top = functools.reduce(jnp.maximum, tops)
        return top, sum(s * jnp.exp2((m - top) * LOG2E) for m, s in zip(tops, sums))

    def exp_sum(ref, m):
        total = jnp.zeros((8, QB), F32)
        for g in range(SUB // 8):
            total = total + jnp.exp2((ref[8 * g:8 * g + 8, :] - m) * LOG2E)
        return total

    per_step = -(-(chips - 1) // (2 * BLOCKS - 2))

    def send_rows(step):
        @pl.loop(0, per_step)
        def _(i):
            c = step * per_step + i + 1

            @pl.when(c < chips)
            def _():
                pltpu.make_async_remote_copy(q_ref, q_all.at[my_row], q_sem.at[0], q_sem.at[1],
                                             device_id=peer(lax.rem(chip + c, chips) * 2 + core), device_id_type=MESH).start()

    @pl.loop(0, BLOCKS)
    def _(k):
        xa[0:128, :] = x_all[pl.ds(row0(k), ob)].reshape(QB, 128).T
        xa[128:144, :] = stack_rows([1.0] * 3, 16, QB).astype(BF16)

        def step(i, carry):
            m, s, m_last = carry
            tops, sums = [m], [s]
            for u in range(UNROLL):
                new, old = (za, zb) if u % 2 == 0 else (zb, za)
                z = logits(i * UNROLL + u)
                new[...] = z
                tops.append(m_last)
                sums.append(exp_sum(old, m_last))
                m_last = functools.reduce(jnp.maximum, [z[8 * g:8 * g + 8, :] for g in range(SUB // 8)])
            return merge(tops, sums) + (m_last,)

        low = jnp.full((8, QB), LOW, F32)
        zb[...] = jnp.full((SUB, QB), LOW, F32)
        m, s, m_last = lax.fori_loop(0, chunks // UNROLL, step, (low, jnp.zeros((8, QB), F32), low))
        m, s = merge([m, m_last], [s, exp_sum(zb, m_last)])
        top = jnp.max(m, axis=0, keepdims=True)
        total = jnp.sum(s * jnp.exp2((m - top) * LOG2E), axis=0, keepdims=True)
        for t in range(2):
            st_send[pl.ds(k * 2 + t, 1)] = jnp.concatenate([top[:, t * 128:(t + 1) * 128], total[:, t * 128:(t + 1) * 128]], axis=0)[None]
        for t in range(2):
            to = stat_owner(k, t, n)

            @pl.when(to != me)
            def _():
                pltpu.make_async_remote_copy(st_send.at[k * 2 + t], st_got.at[me], st_sem.at[0], st_sem.at[1], device_id=peer(to), device_id_type=MESH).start()

            @pl.when(to == me)
            def _():
                st_got[pl.ds(me, 1)] = st_send[pl.ds(k * 2 + t, 1)]

        send_rows(k)
        combine_stats(jnp.where(k == BLOCKS - 1, 2, jnp.where(k < 6, k - 4, -1)))

    drain(lab_all.at[pl.ds(0, n - 1)], lab_sem.at[1])
    swap_q = swap_cores(q_all, swap_sem)

    @pl.loop(0, BLOCKS)
    def _(k):
        send_rows(BLOCKS + k)

        @pl.when(k == BLOCKS - 1)
        def _():
            drain(q_all.at[pl.ds(0, chips - 1)], q_sem.at[1])
            swap_q.start()

        for t in range(2):
            @pl.when(stat_owner(k, t, n) != me)
            def _():
                drain(st_all.at[0], stb_recv.at[k * 2 + t])

        xb[...] = x_all[pl.ds(row0(k), ob)].reshape(QB, 128)
        xa[0:128, :] = xb[...].T
        top = jnp.concatenate([st_all[k * 2, 0:1, :], st_all[k * 2 + 1, 0:1, :]], axis=1)
        norm = jnp.concatenate([st_all[k * 2, 1:2, :], st_all[k * 2 + 1, 1:2, :]], axis=1) + math.log(n * rows)
        xa[128:144, :] = stack_rows([1.0] * 3 + split3(-top) + split3(-norm), 16, QB).astype(BF16)
        lab = jnp.concatenate([jnp.sum(lab_all[pl.ds(row0(k) + t * half, half)], axis=0) for t in range(2)], axis=1) - me * items
        dxt[...] = jnp.zeros_like(dxt)
        gb[...] = jnp.zeros_like(gb)

        zb[...] = jnp.full((SUB, QB), LOW, F32)
        ga[...] = jnp.zeros_like(ga)

        def spread(src, dst, q):
            at = lab - jnp.where(q < 0, -(1 << 29), q * SUB)
            at = jnp.broadcast_to(at, (8, QB))
            tsum = t_acc[...]
            for u in range(SUB // 16):
                parts = []
                for v in range(2):
                    rows8 = pl.ds(u * 16 + v * 8, 8)
                    z = src[rows8, :]
                    idv = ids[rows8, :]
                    hot = jnp.where(jnp.concatenate([idv, idv], axis=1) == at, 1.0 / (n * rows), 0.0)
                    tsum = tsum + z * hot
                    parts.append(jnp.exp2(z * LOG2E) - hot)
                dst[u * 16:(u + 1) * 16, :] = jnp.concatenate(parts, axis=0).astype(BF16)
            t_acc[...] = tsum

        def gather(src, q):
            r = pl.ds(pl.multiple_of(jnp.maximum(q, 0) * SUB, SUB), SUB)
            de_acc[r, :] += jnp.dot(src[...], xb[...], preferred_element_type=F32)
            dxt[...] += jnp.dot(et[:, r], src[...], preferred_element_type=F32)

        @pl.loop(0, chunks // UNROLL)
        def _(i):
            for u in range(UNROLL):
                q = i * UNROLL + u
                new, old = (za, zb) if u % 2 == 0 else (zb, za)
                here, gone = (gb, ga) if u % 2 == 0 else (ga, gb)
                new[...] = logits(q)
                spread(old, here, q - 1)
                gather(gone, q - 2)

        spread(zb, gb, chunks - 1)
        gather(ga, chunks - 2)
        gather(gb, chunks - 1)
        dx_part[pl.ds(k * ob, ob)] = dxt[...].T.reshape(ob, rows, 128)

        pltpu.make_async_remote_copy(dx_part.at[pl.ds(k * ob + (1 - core) * half, half)], pair.at[pl.ds(k * half, half)], pair_send, pair_recv.at[k],
                                     device_id=peer(chip * 2 + 1 - core), device_id_type=MESH).start()

        @pl.when(k > 0)
        def _():
            flush(k - 1)

        combine_stats(k + 3)

        combine_rows(k - 3)

    t_mine[...] = jnp.sum(t_acc[:, 0:128] + t_acc[:, 128:256], axis=0, keepdims=True)
    t_all[pl.ds(me, 1)] = t_mine[...][None]

    @pl.loop(1, n)
    def _(i):
        pltpu.make_async_remote_copy(t_mine, t_all.at[me], t_sem.at[0], t_sem.at[1], device_id=peer(lax.rem(me + i, n)), device_id_type=MESH).start()

    flush(BLOCKS - 1)

    @pl.loop(0, items // 512)
    def _(i):
        r = pl.multiple_of(i * 512, 512)
        de_out[pl.ds(r, 512), :] = de_acc[pl.ds(r, 512), :].astype(BF16)

    out = pltpu.make_async_copy(de_out, de_hbm, out_sem)
    out.start()
    drain(q_all.at[pl.ds(0, chips)], swap_sem.at[1])

    def rows_of(k):
        return q_all[pl.ds(row0(k), ob)].reshape(QB, q_all.shape[-1])

    @pl.loop(0, BLOCKS)
    def _(k):
        pre[pl.ds(k, 1)] = jnp.dot(rows_of(k), w1[...], preferred_element_type=F32)[None]

    def tower(k):
        @pl.when(my_k == k)
        def _():
            if ob > 1:
                drain(dx_all.at[pl.ds(0, ob - 1)], dxb_recv.at[k])

        @pl.when(my_k != k)
        def _():
            drain(dx_all.at[pl.ds(0, ob)], dxb_recv.at[k])

        dx = dx_all[pl.ds(k * ob, ob)].reshape(QB, 128)
        a = pre[k]
        h = jnp.maximum(a, 0.0).astype(BF16)
        acc2[...] += lax.dot_general(h, dx, (((0,), (0,)), ((), ())), preferred_element_type=F32)
        dh = lax.dot_general(dx, w2[...], (((1,), (1,)), ((), ())), preferred_element_type=F32)
        da = jnp.where(a > 0.0, dh, 0.0).astype(BF16)
        acc1[...] += lax.dot_general(rows_of(k), da, (((0,), (0,)), ((), ())), preferred_element_type=F32)

    combine_rows(BLOCKS - 3)
    combine_rows(BLOCKS - 2)
    combine_rows(BLOCKS - 1)
    pl.loop(0, BLOCKS)(tower)
    dw1_ref[...] = acc1[...].astype(BF16)
    dw2_ref[...] = acc2[...].astype(BF16)

    drain(t_all.at[pl.ds(0, n - 1)], t_sem.at[1])
    loss_ref[0] = -jnp.sum(t_all[...]) - math.log(n * rows)

    out.wait()
    swap_q.wait_send()
    swap_x.wait_send()
    drain(x_all.at[pl.ds(0, chips - 1)], x_sem.at[0])
    drain(lab_all.at[pl.ds(0, n - 1)], lab_sem.at[0])
    drain(q_all.at[pl.ds(0, chips - 1)], q_sem.at[0])
    drain(t_all.at[pl.ds(0, n - 1)], t_sem.at[0])
    drain(pair.at[pl.ds(0, BLOCKS * half)], pair_send)

    @pl.when(own_half)
    def _():
        drain(dx_got.at[pl.ds(0, chips - 1)], dx_sem.at[0])

    @pl.when(jnp.logical_not(own_half))
    def _():
        drain(dx_got.at[pl.ds(0, chips)], dx_sem.at[0])

    @pl.when(is_stat)
    def _():
        drain(st_got.at[pl.ds(0, n - 1)], stb_send)
        drain(st_got.at[pl.ds(0, 2 * BLOCKS - 1)], st_sem.at[0])

    @pl.when(jnp.logical_not(is_stat))
    def _():
        drain(st_got.at[pl.ds(0, 2 * BLOCKS)], st_sem.at[0])

    drain(dx_all.at[pl.ds(0, n - 1)], dxb_send)


def store_kernel(pieces, *refs):
    count = len(pieces)
    ins, outs, bufs, in_sem, out_sem = refs[:count], refs[count:2 * count], refs[2 * count:3 * count], refs[-2], refs[-1]
    reads, writes = [], []
    for a, o, v, p in zip(ins, outs, bufs, pieces):
        step = a.shape[0] // p
        for i in range(p):
            part = pl.ds(i * step, step)
            at = len(reads)
            reads.append(pltpu.make_async_copy(a.at[part], v.at[part], in_sem.at[at]))
            writes.append(pltpu.make_async_copy(v.at[part], o.at[part], out_sem.at[at]))
    for c in reads:
        c.start()
    for r, w in zip(reads, writes):
        r.wait()
        w.start()
    for w in writes:
        w.wait()


def store(*arrays):
    pieces = (4, 2, 1)
    any_space = pl.BlockSpec(memory_space=pl.ANY)
    return pl.pallas_call(
        functools.partial(store_kernel, pieces),
        name="store",
        out_shape=tuple(jax.ShapeDtypeStruct(a.shape, a.dtype) for a in arrays),
        in_specs=[any_space] * 3,
        out_specs=(any_space,) * 3,
        scratch_shapes=[pltpu.VMEM(a.shape, a.dtype) for a in arrays] + [DMA((sum(pieces),)), DMA((sum(pieces),))],
        compiler_params=pltpu.CompilerParams(vmem_limit_bytes=60 << 20),
    )(*arrays)


def solution(mesh):
    n = mesh.shape["tp"]

    def local_step(queries, w_first, w_second, catalogue, log_q, labels):
        rows, width = queries.shape
        items = catalogue.shape[0]
        hidden = w_first.shape[1]
        ob = n // BLOCKS
        V, ANY = pl.BlockSpec(memory_space=pltpu.VMEM), pl.BlockSpec(memory_space=pl.ANY)
        S = jax.ShapeDtypeStruct
        M = pltpu.VMEM
        i32 = jnp.int32
        loss, grad_items, grad_first, grad_second = pl.pallas_call(
            functools.partial(kernel, n, rows, items),
            name="two_tower",
            out_shape=(S((1,), F32), S((items, 128), BF16), S((width, hidden), BF16), S((hidden, 128), BF16)),
            in_specs=[V, ANY, ANY, ANY, V, V],
            out_specs=(pl.BlockSpec(memory_space=pltpu.SMEM), ANY, V, V),
            scratch_shapes=[
                M((width, hidden), BF16), M((hidden, 128), BF16), M((items, 256), BF16), M((128, items), BF16), M((SUB, 128), i32),
                M((rows, 128), BF16), M((1, 128), i32), M((n, rows, 128), BF16), M((n, 1, 128), i32), M((n, rows, width), BF16), M((256, QB), BF16), M((QB, 128), BF16), M((SUB, QB), F32), M((SUB, QB), F32), M((SUB, QB), BF16), M((SUB, QB), BF16),
                M((2 * BLOCKS, 2, 128), F32), M((n, 2, 128), F32), M((2, 128), F32), M((2 * BLOCKS, 2, 128), F32), M((items, 128), F32), M((items, 128), BF16), M((128, QB), F32),
                M((n, rows, 128), F32), M((n // 2, rows, 128), F32), M((n // 2, rows, 128), F32), M((n // 2, rows, 128), F32), M((rows, 128), BF16), M((n, rows, 128), BF16),
                M((8, QB), F32), M((1, 128), F32), M((n, 1, 128), F32), M((BLOCKS, QB, hidden), F32), M((width, hidden), F32), M((hidden, 128), F32),
                DMA((3,)), DMA, DMA((2,)), DMA((2,)), DMA((2,)), DMA((2,)), DMA((2,)), DMA((2,)), DMA, DMA((2 * BLOCKS,)), DMA, DMA((BLOCKS,)), DMA((2,)), DMA, DMA((BLOCKS,)), DMA((2,)),
            ],
            compiler_params=pltpu.CompilerParams(collective_id=0, has_side_effects=True, vmem_limit_bytes=60 << 20),
        )(queries, w_first, w_second, catalogue, log_q.reshape(items // 128, 128), labels.reshape(1, rows))
        return (loss,) + tuple(store(grad_items, grad_first, grad_second))

    row_spec = P(("dp", "tp"), None)
    return jax.shard_map(local_step, mesh=mesh, in_specs=(row_spec, P(None, None), P(None, None), P("tp", None), P("tp"), P(("dp", "tp"))), out_specs=(P("dp"), row_spec, P("dp", None), P("dp", None)), check_vma=False)
```

```python
import functools
import math
import jax
import jax.numpy as jnp
from jax import lax
from jax.experimental import pallas as pl
from jax.experimental.pallas import tpu as pltpu
from jax.sharding import PartitionSpec as P

MESH = pl.DeviceIdType.MESH
DMA = pltpu.SemaphoreType.DMA
F32, BF16 = jnp.float32, jnp.bfloat16
LOG2E = 1.4426950408889634
BLOCKS = 8
QB = 256
SUB = 512
KEEP = 3


def peer(index):
    return {"tp": index}


def drain(ref, sem):
    pltpu.make_async_copy(ref, ref, sem).wait()


def slot_of(d, n):
    core, chip = d % 2, d // 2
    if n == 128:
        x, y, z = chip % 4, (chip // 4) % 4, chip // 16
        return ((x + y + z) % 4) * 2 + core, z * 4 + y
    return (chip % 4) * 2 + core, chip // 4


def device_of(k, j, n):
    if n == 128:
        z, y = j // 4, j % 4
        x = (k // 2 + 8 - y - z) % 4
        return ((z * 4 + y) * 4 + x) * 2 + k % 2
    return (j * 4 + k // 2) * 2 + k % 2


def each(first, count, f):
    steps = (count - first) // 4

    @pl.loop(0, steps)
    def _(s):
        for u in range(4):
            f(first + s * 4 + u)

    for i in range(first + steps * 4, count):
        f(i)


def split3(v):
    big = float(jnp.finfo(BF16).max)
    a = jnp.clip(v, -big, big).astype(BF16).astype(F32)
    b = (v - a).astype(BF16).astype(F32)
    return [a, b, v - a - b]


def stack_rows(values, height, width=128):
    at = lax.broadcasted_iota(jnp.int32, (height, width), 0)
    out = jnp.zeros((height, width), F32)
    for i, v in enumerate(values):
        out = jnp.where(at == i, v, out)
    return out


def stat_owner(k, t, n):
    return device_of(5, 2 * k + t, n) if n == 128 else device_of(k, t * (n // BLOCKS // 2), n)


def kernel(n, rows, items,
           q_ref, w1_hbm, w2_hbm, e_hbm, lq_ref, lab_ref,
           loss_ref, de_hbm, dw1_ref, dw2_ref,
           w1, w2, e, et, ids, x_mine, lab_mine, x_all, lab_all, q_all, xa, xb, za, zb, ga, gb, keep, xk,
           st_send, st_got, st_mine, st_all, de_acc, de_out, dxt, dx_part, pair, dx_sum, dx_got, dx_mine, dx_all,
           t_acc, t_mine, t_all, pre, acc1, acc2,
           load_sem, out_sem, x_sem, xs_sem, lab_sem, q_sem, swap_sem, st_sem, stb_send, stb_recv, pair_send, pair_recv, dx_sem, dxb_send, dxb_recv, t_sem):
    me = lax.axis_index("tp")
    ob = n // BLOCKS
    half = ob // 2
    my_k, my_j = slot_of(me, n)
    my_slot = my_k * ob + my_j
    core, chip, chips = me % 2, me // 2, n // 2
    my_row = core * chips + (my_k // 2) * ob + my_j

    if n == 128:
        is_stat, stat_k, stat_t = my_k == 5, my_j // 2, my_j % 2
    else:
        is_stat, stat_k, stat_t = my_j % half == 0, my_k, my_j // half

    def row0(k):
        return (k % 2) * chips + (k // 2) * ob

    def swap_cores(ref, sem):
        part = ref.at[pl.ds(core * chips, chips)]
        return pltpu.make_async_remote_copy(part, part, sem.at[0], sem.at[1], device_id=peer(chip * 2 + 1 - core), device_id_type=MESH)

    loads = [pltpu.make_async_copy(a, b, load_sem.at[i]) for i, (a, b) in enumerate(((w1_hbm, w1), (w2_hbm, w2), (e_hbm, e.at[:, 0:128])))]
    for c in loads:
        c.start()
    barrier = pltpu.get_barrier_semaphore()

    each(1, n, lambda k: pl.semaphore_signal(barrier, inc=1, device_id=peer(lax.rem(me + k, n)), device_id_type=MESH))

    loads[0].wait()
    loads[1].wait()
    hid = jnp.maximum(jnp.dot(q_ref[...], w1[...], preferred_element_type=F32), 0.0).astype(BF16)
    x_mine[...] = jnp.dot(hid, w2[...], preferred_element_type=F32).astype(BF16)
    lanes = lax.broadcasted_iota(jnp.int32, (1, 128), 1)
    wide = jnp.concatenate([lab_ref[...]] * (128 // rows), axis=1) if rows < 128 else lab_ref[...]
    lab_mine[...] = jnp.where(lanes // rows == my_j % half, wide, 0)
    x_all[pl.ds(my_row, 1)] = x_mine[...][None]
    lab_all[pl.ds(my_row, 1)] = lab_mine[...][None]
    q_all[pl.ds(my_row, 1)] = q_ref[...][None]
    loads[2].wait()

    @pl.loop(0, items // 1024)
    def _(i):
        parts = split3(-lq_ref[pl.ds(pl.multiple_of(i * 8, 8), 8), :])
        for u in range(8):
            r = pl.multiple_of(i * 1024 + u * 128, 128)
            extra = stack_rows([p[u:u + 1, :] for p in parts] + [1.0] * 6, 16)
            e[pl.ds(r, 128), 128:256] = jnp.concatenate([extra, jnp.zeros((112, 128), F32)], axis=0).T.astype(BF16)
            et[:, pl.ds(r, 128)] = e[pl.ds(r, 128), 0:128].T
            de_acc[pl.ds(r, 128), :] = jnp.zeros((128, 128), F32)

    ids[...] = lax.broadcasted_iota(jnp.int32, (SUB, 128), 0)
    xa[144:256, :] = jnp.zeros((112, QB), BF16)
    t_acc[...] = jnp.zeros_like(t_acc)
    acc1[...] = jnp.zeros_like(acc1)
    acc2[...] = jnp.zeros_like(acc2)
    pl.semaphore_wait(barrier, n - 1)

    def send_x(k):
        to = peer(lax.rem(chip + k, chips) * 2 + core)
        pltpu.make_async_remote_copy(x_mine, x_all.at[my_row], x_sem.at[0], x_sem.at[1], device_id=to, device_id_type=MESH).start()

    def send_labels(k):
        to = peer(lax.rem(me + k, n))
        pltpu.make_async_remote_copy(lab_mine, lab_all.at[my_row], lab_sem.at[0], lab_sem.at[1], device_id=to, device_id_type=MESH).start()

    each(1, chips, send_x)
    each(1, n, send_labels)
    drain(x_all.at[pl.ds(0, chips - 1)], x_sem.at[1])
    swap_x = swap_cores(x_all, xs_sem)
    swap_x.start()
    drain(x_all.at[pl.ds(0, chips)], xs_sem.at[1])


    def combine_stats(k):
        @pl.when(jnp.logical_and(is_stat, stat_k == k))
        def _():
            drain(st_got.at[pl.ds(0, n - 1)], st_sem.at[1])
            top = jnp.max(st_got[:, 0:1, :], axis=0)
            total = jnp.sum(st_got[:, 1:2, :] * jnp.exp(st_got[:, 0:1, :] - top[None]), axis=0)
            st_mine[...] = jnp.concatenate([top, jnp.log(total)], axis=0)
            st_all[pl.ds(k * 2 + stat_t, 1)] = st_mine[...][None]

            def send(i):
                pltpu.make_async_remote_copy(st_mine, st_all.at[k * 2 + stat_t], stb_send, stb_recv.at[k * 2 + stat_t],
                                             device_id=peer(lax.rem(me + i, n)), device_id_type=MESH).start()

            each(1, n, send)

    def flush(k):
        drain(pair.at[pl.ds(0, half)], pair_recv.at[k])
        dx_sum[pl.ds(k * half, half)] = dx_part[pl.ds(k * ob + core * half, half)] + pair[pl.ds(k * half, half)]

        @pl.loop(0, half)
        def _(j):
            to = device_of(k, core * half + j, n)

            @pl.when(to != me)
            def _():
                pltpu.make_async_remote_copy(dx_sum.at[k * half + j], dx_got.at[chip], dx_sem.at[0], dx_sem.at[1], device_id=peer(to), device_id_type=MESH).start()

            @pl.when(to == me)
            def _():
                dx_got[pl.ds(chip, 1)] = dx_sum[pl.ds(k * half + j, 1)]

    own_half = my_j // half == core

    def combine_rows(k):
        @pl.when(my_k == k)
        def _():
            @pl.when(own_half)
            def _():
                drain(dx_got.at[pl.ds(0, chips - 1)], dx_sem.at[1])

            @pl.when(jnp.logical_not(own_half))
            def _():
                drain(dx_got.at[pl.ds(0, chips)], dx_sem.at[1])

            dx_mine[...] = jnp.sum(dx_got[...], axis=0).astype(BF16)
            dx_all[pl.ds(my_slot, 1)] = dx_mine[...][None]

            def send(i):
                pltpu.make_async_remote_copy(dx_mine, dx_all.at[my_slot], dxb_send, dxb_recv.at[k],
                                             device_id=peer(lax.rem(me + i, n)), device_id_type=MESH).start()

            each(1, n, send)

    def logits(q):
        return jnp.dot(e[pl.ds(q * SUB, SUB), :], xa[...], preferred_element_type=F32)

    chunks = items // SUB

    def merge(tops, sums):
        top = functools.reduce(jnp.maximum, tops)
        return top, sum(s * jnp.exp2((m - top) * LOG2E) for m, s in zip(tops, sums))

    def exp_sum(ref, m):
        total = jnp.zeros((8, QB), F32)
        for g in range(SUB // 64):
            z = ref[64 * g:64 * g + 64, :].reshape(8, 8, QB)
            total = total + jnp.sum(jnp.exp2((z - m[None]) * LOG2E), axis=0)
        return total

    per_step = -(-(chips - 1) // (2 * BLOCKS - 2))

    def send_rows(step):
        @pl.loop(0, per_step)
        def _(i):
            c = step * per_step + i + 1

            @pl.when(c < chips)
            def _():
                pltpu.make_async_remote_copy(q_ref, q_all.at[my_row], q_sem.at[0], q_sem.at[1],
                                             device_id=peer(lax.rem(chip + c, chips) * 2 + core), device_id_type=MESH).start()

    @pl.loop(0, BLOCKS)
    def _(k):
        xa[0:128, :] = x_all[pl.ds(row0(k), ob)].reshape(QB, 128).T
        xa[128:144, :] = stack_rows([1.0] * 3, 16, QB).astype(BF16)

        m = s = None
        tops, sums = [], []
        for q in range(chunks + 1):
            new, old = (za, zb) if q % 2 == 0 else (zb, za)
            if q < chunks:
                z = logits(q)
                new[...] = z
            if q > 0:
                sums.append(exp_sum(old, tops[len(sums)]))
            if q < chunks:
                tops.append(jnp.max(z.reshape(SUB // 8, 8, QB), axis=0))
            if len(sums) == 4 or q == chunks:
                done = len(sums)
                old_parts = ([m], [s]) if m is not None else ([], [])
                m, s = merge(old_parts[0] + tops[:done], old_parts[1] + sums)
                tops, sums = tops[done:], []
        top = jnp.max(m, axis=0, keepdims=True)
        total = jnp.sum(s * jnp.exp2((m - top) * LOG2E), axis=0, keepdims=True)
        for t in range(2):
            st_send[pl.ds(k * 2 + t, 1)] = jnp.concatenate([top[:, t * 128:(t + 1) * 128], total[:, t * 128:(t + 1) * 128]], axis=0)[None]
        for t in range(2):
            to = stat_owner(k, t, n)

            @pl.when(to != me)
            def _():
                pltpu.make_async_remote_copy(st_send.at[k * 2 + t], st_got.at[me], st_sem.at[0], st_sem.at[1], device_id=peer(to), device_id_type=MESH).start()

            @pl.when(to == me)
            def _():
                st_got[pl.ds(me, 1)] = st_send[pl.ds(k * 2 + t, 1)]

        send_rows(k)
        combine_stats(jnp.where(k == BLOCKS - 1, 2, jnp.where(k < 6, k - 4, -1)))

    drain(lab_all.at[pl.ds(0, n - 1)], lab_sem.at[1])
    swap_q = swap_cores(q_all, swap_sem)

    def grads(k, kept):
        send_rows(BLOCKS + k)

        @pl.when(k == BLOCKS - 1)
        def _():
            drain(q_all.at[pl.ds(0, chips - 1)], q_sem.at[1])
            swap_q.start()

        for t in range(2):
            @pl.when(stat_owner(k, t, n) != me)
            def _():
                drain(st_all.at[0], stb_recv.at[k * 2 + t])

        xb[...] = x_all[pl.ds(row0(k), ob)].reshape(QB, 128)
        xa[0:128, :] = xb[...].T
        top = jnp.concatenate([st_all[k * 2, 0:1, :], st_all[k * 2 + 1, 0:1, :]], axis=1)
        norm = jnp.concatenate([st_all[k * 2, 1:2, :], st_all[k * 2 + 1, 1:2, :]], axis=1) + math.log(n * rows)
        xa[128:144, :] = stack_rows([1.0] * 3 + split3(-top) + split3(-norm), 16, QB).astype(BF16)
        lab = jnp.concatenate([jnp.sum(lab_all[pl.ds(row0(k) + t * half, half)], axis=0) for t in range(2)], axis=1) - me * items
        dxt[...] = jnp.zeros_like(dxt)
        gb[...] = jnp.zeros_like(gb)


        def spread(src, dst, q):
            tsum = t_acc[...]
            for u in range(SUB // 64):
                part = pl.ds(u * 64, 64)
                z = src[part, :]
                idv = ids[part, :]
                hot = jnp.where(jnp.concatenate([idv, idv], axis=1) == lab - q * SUB, 1.0 / (n * rows), 0.0)
                tsum = tsum + jnp.sum((z * hot).reshape(8, 8, QB), axis=0)
                dst[part, :] = (jnp.exp2(z * LOG2E) - hot).astype(BF16)
            t_acc[...] = tsum

        for q in range(chunks + 2):
            if q < chunks:
                (za if q % 2 == 0 else zb)[...] = logits(q)
            if 0 < q <= chunks:
                to = ga if q % 2 else gb
                spread(zb if q % 2 == 0 else za, to if kept is None else keep.at[kept, pl.ds((q - 1) * SUB, SUB)], q - 1)
            if q > 1:
                r = pl.ds((q - 2) * SUB, SUB)
                g = (gb if q % 2 else ga)[...] if kept is None else keep[kept, r, :]
                if kept is None:
                    de_acc[r, :] += jnp.dot(g, xb[...], preferred_element_type=F32)
                dxt[...] += jnp.dot(et[:, r], g, preferred_element_type=F32)

        dx_part[pl.ds(k * ob, ob)] = dxt[...].T.reshape(ob, rows, 128)

        pltpu.make_async_remote_copy(dx_part.at[pl.ds(k * ob + (1 - core) * half, half)], pair.at[pl.ds(k * half, half)], pair_send, pair_recv.at[k],
                                     device_id=peer(chip * 2 + 1 - core), device_id_type=MESH).start()

        @pl.when(k > 0)
        def _():
            flush(k - 1)

        combine_stats(k + 3)

        combine_rows(k - 3)

    pl.loop(0, BLOCKS - KEEP)(lambda k: grads(k, None))
    pl.loop(BLOCKS - KEEP, BLOCKS)(lambda k: grads(k, k - (BLOCKS - KEEP)))

    t_mine[...] = jnp.sum(t_acc[:, 0:128] + t_acc[:, 128:256], axis=0, keepdims=True)
    t_all[pl.ds(me, 1)] = t_mine[...][None]

    def send_t(i):
        pltpu.make_async_remote_copy(t_mine, t_all.at[me], t_sem.at[0], t_sem.at[1], device_id=peer(lax.rem(me + i, n)), device_id_type=MESH).start()

    each(1, n, send_t)

    flush(BLOCKS - 1)

    for i in range(KEEP):
        xk[pl.ds(i * QB, QB), :] = x_all[pl.ds(row0(BLOCKS - KEEP + i), ob)].reshape(QB, 128)

    @pl.loop(0, items // 512)
    def _(i):
        r = pl.ds(pl.multiple_of(i * 512, 512), 512)
        g = jnp.concatenate([keep[b, r, :] for b in range(KEEP)], axis=1)
        de_out[r, :] = (de_acc[r, :] + jnp.dot(g, xk[...], preferred_element_type=F32)).astype(BF16)

    out = pltpu.make_async_copy(de_out, de_hbm, out_sem)
    out.start()
    drain(q_all.at[pl.ds(0, chips)], swap_sem.at[1])

    def rows_of(k):
        return q_all[pl.ds(row0(k), ob)].reshape(QB, q_all.shape[-1])

    @pl.loop(0, BLOCKS)
    def _(k):
        pre[pl.ds(k, 1)] = jnp.dot(rows_of(k), w1[...], preferred_element_type=F32)[None]

    def tower(k):
        @pl.when(my_k == k)
        def _():
            if ob > 1:
                drain(dx_all.at[pl.ds(0, ob - 1)], dxb_recv.at[k])

        @pl.when(my_k != k)
        def _():
            drain(dx_all.at[pl.ds(0, ob)], dxb_recv.at[k])

        dx = dx_all[pl.ds(k * ob, ob)].reshape(QB, 128)
        a = pre[k]
        h = jnp.maximum(a, 0.0).astype(BF16)
        acc2[...] += lax.dot_general(h, dx, (((0,), (0,)), ((), ())), preferred_element_type=F32)
        dh = lax.dot_general(dx, w2[...], (((1,), (1,)), ((), ())), preferred_element_type=F32)
        da = jnp.where(a > 0.0, dh, 0.0).astype(BF16)
        acc1[...] += lax.dot_general(rows_of(k), da, (((0,), (0,)), ((), ())), preferred_element_type=F32)

    combine_rows(BLOCKS - 3)
    combine_rows(BLOCKS - 2)
    combine_rows(BLOCKS - 1)
    pl.loop(0, BLOCKS)(tower)
    dw1_ref[...] = acc1[...].astype(BF16)
    dw2_ref[...] = acc2[...].astype(BF16)

    drain(t_all.at[pl.ds(0, n - 1)], t_sem.at[1])
    loss_ref[0] = -jnp.sum(t_all[...]) - math.log(n * rows)

    out.wait()
    swap_q.wait_send()
    swap_x.wait_send()
    drain(x_all.at[pl.ds(0, chips - 1)], x_sem.at[0])
    drain(lab_all.at[pl.ds(0, n - 1)], lab_sem.at[0])
    drain(q_all.at[pl.ds(0, chips - 1)], q_sem.at[0])
    drain(t_all.at[pl.ds(0, n - 1)], t_sem.at[0])
    drain(pair.at[pl.ds(0, BLOCKS * half)], pair_send)

    @pl.when(own_half)
    def _():
        drain(dx_got.at[pl.ds(0, chips - 1)], dx_sem.at[0])

    @pl.when(jnp.logical_not(own_half))
    def _():
        drain(dx_got.at[pl.ds(0, chips)], dx_sem.at[0])

    @pl.when(is_stat)
    def _():
        drain(st_got.at[pl.ds(0, n - 1)], stb_send)
        drain(st_got.at[pl.ds(0, 2 * BLOCKS - 1)], st_sem.at[0])

    @pl.when(jnp.logical_not(is_stat))
    def _():
        drain(st_got.at[pl.ds(0, 2 * BLOCKS)], st_sem.at[0])

    drain(dx_all.at[pl.ds(0, n - 1)], dxb_send)


def store_kernel(pieces, *refs):
    count = len(pieces)
    ins, outs, bufs, in_sem, out_sem = refs[:count], refs[count:2 * count], refs[2 * count:3 * count], refs[-2], refs[-1]
    reads, writes = [], []
    for a, o, v, p in zip(ins, outs, bufs, pieces):
        step = a.shape[0] // p
        for i in range(p):
            part = pl.ds(i * step, step)
            at = len(reads)
            reads.append(pltpu.make_async_copy(a.at[part], v.at[part], in_sem.at[at]))
            writes.append(pltpu.make_async_copy(v.at[part], o.at[part], out_sem.at[at]))
    for c in reads:
        c.start()
    for r, w in zip(reads, writes):
        r.wait()
        w.start()
    for w in writes:
        w.wait()


def store(*arrays):
    pieces = (4, 2, 1)
    any_space = pl.BlockSpec(memory_space=pl.ANY)
    return pl.pallas_call(
        functools.partial(store_kernel, pieces),
        name="store",
        out_shape=tuple(jax.ShapeDtypeStruct(a.shape, a.dtype) for a in arrays),
        in_specs=[any_space] * 3,
        out_specs=(any_space,) * 3,
        scratch_shapes=[pltpu.VMEM(a.shape, a.dtype) for a in arrays] + [DMA((sum(pieces),)), DMA((sum(pieces),))],
        compiler_params=pltpu.CompilerParams(vmem_limit_bytes=60 << 20),
    )(*arrays)


def solution(mesh):
    n = mesh.shape["tp"]

    def local_step(queries, w_first, w_second, catalogue, log_q, labels):
        rows, width = queries.shape
        items = catalogue.shape[0]
        hidden = w_first.shape[1]
        ob = n // BLOCKS
        V, ANY = pl.BlockSpec(memory_space=pltpu.VMEM), pl.BlockSpec(memory_space=pl.ANY)
        S = jax.ShapeDtypeStruct
        M = pltpu.VMEM
        i32 = jnp.int32
        loss, grad_items, grad_first, grad_second = pl.pallas_call(
            functools.partial(kernel, n, rows, items),
            name="two_tower",
            out_shape=(S((1,), F32), S((items, 128), BF16), S((width, hidden), BF16), S((hidden, 128), BF16)),
            in_specs=[V, ANY, ANY, ANY, V, V],
            out_specs=(pl.BlockSpec(memory_space=pltpu.SMEM), ANY, V, V),
            scratch_shapes=[
                M((width, hidden), BF16), M((hidden, 128), BF16), M((items, 256), BF16), M((128, items), BF16), M((SUB, 128), i32),
                M((rows, 128), BF16), M((1, 128), i32), M((n, rows, 128), BF16), M((n, 1, 128), i32), M((n, rows, width), BF16), M((256, QB), BF16), M((QB, 128), BF16), M((SUB, QB), F32), M((SUB, QB), F32), M((SUB, QB), BF16), M((SUB, QB), BF16), M((KEEP, items, QB), BF16), M((KEEP * QB, 128), BF16),
                M((2 * BLOCKS, 2, 128), F32), M((n, 2, 128), F32), M((2, 128), F32), M((2 * BLOCKS, 2, 128), F32), M((items, 128), F32), M((items, 128), BF16), M((128, QB), F32),
                M((n, rows, 128), F32), M((n // 2, rows, 128), F32), M((n // 2, rows, 128), F32), M((n // 2, rows, 128), F32), M((rows, 128), BF16), M((n, rows, 128), BF16),
                M((8, QB), F32), M((1, 128), F32), M((n, 1, 128), F32), M((BLOCKS, QB, hidden), F32), M((width, hidden), F32), M((hidden, 128), F32),
                DMA((3,)), DMA, DMA((2,)), DMA((2,)), DMA((2,)), DMA((2,)), DMA((2,)), DMA((2,)), DMA, DMA((2 * BLOCKS,)), DMA, DMA((BLOCKS,)), DMA((2,)), DMA, DMA((BLOCKS,)), DMA((2,)),
            ],
            compiler_params=pltpu.CompilerParams(collective_id=0, has_side_effects=True, vmem_limit_bytes=60 << 20),
        )(queries, w_first, w_second, catalogue, log_q.reshape(items // 128, 128), labels.reshape(1, rows))
        return (loss,) + tuple(store(grad_items, grad_first, grad_second))

    row_spec = P(("dp", "tp"), None)
    return jax.shard_map(local_step, mesh=mesh, in_specs=(row_spec, P(None, None), P(None, None), P("tp", None), P("tp"), P(("dp", "tp"))), out_specs=(P("dp"), row_spec, P("dp", None), P("dp", None)), check_vma=False)
```

```python
import functools
import math
import jax
import jax.numpy as jnp
from jax import lax
from jax.experimental import pallas as pl
from jax.experimental.pallas import tpu as pltpu
from jax.sharding import PartitionSpec as P

MESH = pl.DeviceIdType.MESH
DMA = pltpu.SemaphoreType.DMA
F32, BF16 = jnp.float32, jnp.bfloat16
LOG2E = 1.4426950408889634
BLOCKS = 8
QB = 256
SUB = 512
KEEP = 1


def peer(index):
    return {"tp": index}


def drain(ref, sem):
    pltpu.make_async_copy(ref, ref, sem).wait()


def slot_of(d, n):
    core, chip = d % 2, d // 2
    if n == 128:
        x, y, z = chip % 4, (chip // 4) % 4, chip // 16
        return ((x + y + z) % 4) * 2 + core, z * 4 + y
    return (chip % 4) * 2 + core, chip // 4


def device_of(k, j, n):
    if n == 128:
        z, y = j // 4, j % 4
        x = (k // 2 + 8 - y - z) % 4
        return ((z * 4 + y) * 4 + x) * 2 + k % 2
    return (j * 4 + k // 2) * 2 + k % 2


def each(first, count, f):
    steps = (count - first) // 4

    @pl.loop(0, steps)
    def _(s):
        for u in range(4):
            f(first + s * 4 + u)

    for i in range(first + steps * 4, count):
        f(i)


def split3(v):
    big = float(jnp.finfo(BF16).max)
    a = jnp.clip(v, -big, big).astype(BF16).astype(F32)
    b = (v - a).astype(BF16).astype(F32)
    return [a, b, v - a - b]


def stack_rows(values, height, width=128):
    at = lax.broadcasted_iota(jnp.int32, (height, width), 0)
    out = jnp.zeros((height, width), F32)
    for i, v in enumerate(values):
        out = jnp.where(at == i, v, out)
    return out


def stat_owner(k, t, n):
    return device_of(5, 2 * k + t, n) if n == 128 else device_of(k, t * (n // BLOCKS // 2), n)


def kernel(n, rows, items,
           q_ref, w1_hbm, w2_hbm, e_hbm, lq_ref, lab_ref,
           loss_ref, de_hbm, dw1_ref, dw2_ref,
           w1, w2, e, et, ids, x_mine, lab_mine, x_all, lab_all, q_all, xa, xb, za, zb, ga, gb, keep, xk,
           st_send, st_got, st_mine, st_all, de_acc, de_out, dxt, dx_part, pair, dx_sum, dx_got, dx_mine, dx_all,
           t_acc, t_mine, t_all, pre, acc1, acc2,
           load_sem, out_sem, x_sem, xs_sem, lab_sem, q_sem, swap_sem, st_sem, stb_send, stb_recv, pair_send, pair_recv, dx_sem, dxb_send, dxb_recv, t_sem):
    me = lax.axis_index("tp")
    ob = n // BLOCKS
    half = ob // 2
    my_k, my_j = slot_of(me, n)
    my_slot = my_k * ob + my_j
    core, chip, chips = me % 2, me // 2, n // 2
    my_row = core * chips + (my_k // 2) * ob + my_j

    if n == 128:
        is_stat, stat_k, stat_t = my_k == 5, my_j // 2, my_j % 2
    else:
        is_stat, stat_k, stat_t = my_j % half == 0, my_k, my_j // half

    def row0(k):
        return (k % 2) * chips + (k // 2) * ob

    def swap_cores(ref, sem):
        part = ref.at[pl.ds(core * chips, chips)]
        return pltpu.make_async_remote_copy(part, part, sem.at[0], sem.at[1], device_id=peer(chip * 2 + 1 - core), device_id_type=MESH)

    loads = [pltpu.make_async_copy(a, b, load_sem.at[i]) for i, (a, b) in enumerate(((w1_hbm, w1), (w2_hbm, w2), (e_hbm, e.at[:, 0:128])))]
    for c in loads:
        c.start()
    barrier = pltpu.get_barrier_semaphore()

    each(1, n, lambda k: pl.semaphore_signal(barrier, inc=1, device_id=peer(lax.rem(me + k, n)), device_id_type=MESH))

    loads[0].wait()
    loads[1].wait()
    hid = jnp.maximum(jnp.dot(q_ref[...], w1[...], preferred_element_type=F32), 0.0).astype(BF16)
    x_mine[...] = jnp.dot(hid, w2[...], preferred_element_type=F32).astype(BF16)
    lanes = lax.broadcasted_iota(jnp.int32, (1, 128), 1)
    wide = jnp.concatenate([lab_ref[...]] * (128 // rows), axis=1) if rows < 128 else lab_ref[...]
    lab_mine[...] = jnp.where(lanes // rows == my_j % half, wide, 0)
    x_all[pl.ds(my_row, 1)] = x_mine[...][None]
    lab_all[pl.ds(my_row, 1)] = lab_mine[...][None]
    q_all[pl.ds(my_row, 1)] = q_ref[...][None]
    loads[2].wait()

    @pl.loop(0, items // 1024)
    def _(i):
        parts = split3(-lq_ref[pl.ds(pl.multiple_of(i * 8, 8), 8), :])
        for u in range(8):
            r = pl.multiple_of(i * 1024 + u * 128, 128)
            extra = stack_rows([p[u:u + 1, :] for p in parts] + [1.0] * 6, 16)
            e[pl.ds(r, 128), 128:256] = jnp.concatenate([extra, jnp.zeros((112, 128), F32)], axis=0).T.astype(BF16)
            et[:, pl.ds(r, 128)] = e[pl.ds(r, 128), 0:128].T
            de_acc[pl.ds(r, 128), :] = jnp.zeros((128, 128), F32)

    ids[...] = lax.broadcasted_iota(jnp.int32, (SUB, 128), 0)
    xa[144:256, :] = jnp.zeros((112, QB), BF16)
    t_acc[...] = jnp.zeros_like(t_acc)
    acc1[...] = jnp.zeros_like(acc1)
    acc2[...] = jnp.zeros_like(acc2)
    pl.semaphore_wait(barrier, n - 1)

    def send_x(k):
        to = peer(lax.rem(chip + k, chips) * 2 + core)
        pltpu.make_async_remote_copy(x_mine, x_all.at[my_row], x_sem.at[0], x_sem.at[1], device_id=to, device_id_type=MESH).start()

    def send_labels(k):
        to = peer(lax.rem(me + k, n))
        pltpu.make_async_remote_copy(lab_mine, lab_all.at[my_row], lab_sem.at[0], lab_sem.at[1], device_id=to, device_id_type=MESH).start()

    each(1, chips, send_x)
    each(1, n, send_labels)
    drain(x_all.at[pl.ds(0, chips - 1)], x_sem.at[1])
    swap_x = swap_cores(x_all, xs_sem)
    swap_x.start()
    drain(x_all.at[pl.ds(0, chips)], xs_sem.at[1])


    def combine_stats(k):
        @pl.when(jnp.logical_and(is_stat, stat_k == k))
        def _():
            drain(st_got.at[pl.ds(0, n - 1)], st_sem.at[1])
            top = jnp.max(st_got[:, 0:1, :], axis=0)
            total = jnp.sum(st_got[:, 1:2, :] * jnp.exp(st_got[:, 0:1, :] - top[None]), axis=0)
            st_mine[...] = jnp.concatenate([top, jnp.log(total)], axis=0)
            st_all[pl.ds(k * 2 + stat_t, 1)] = st_mine[...][None]

            def send(i):
                pltpu.make_async_remote_copy(st_mine, st_all.at[k * 2 + stat_t], stb_send, stb_recv.at[k * 2 + stat_t],
                                             device_id=peer(lax.rem(me + i, n)), device_id_type=MESH).start()

            each(1, n, send)

    def flush(k):
        drain(pair.at[pl.ds(0, half)], pair_recv.at[k])
        dx_sum[pl.ds(k * half, half)] = dx_part[pl.ds(k * ob + core * half, half)] + pair[pl.ds(k * half, half)]

        @pl.loop(0, half)
        def _(j):
            to = device_of(k, core * half + j, n)

            @pl.when(to != me)
            def _():
                pltpu.make_async_remote_copy(dx_sum.at[k * half + j], dx_got.at[chip], dx_sem.at[0], dx_sem.at[1], device_id=peer(to), device_id_type=MESH).start()

            @pl.when(to == me)
            def _():
                dx_got[pl.ds(chip, 1)] = dx_sum[pl.ds(k * half + j, 1)]

    own_half = my_j // half == core

    def combine_rows(k):
        @pl.when(my_k == k)
        def _():
            @pl.when(own_half)
            def _():
                drain(dx_got.at[pl.ds(0, chips - 1)], dx_sem.at[1])

            @pl.when(jnp.logical_not(own_half))
            def _():
                drain(dx_got.at[pl.ds(0, chips)], dx_sem.at[1])

            dx_mine[...] = jnp.sum(dx_got[...], axis=0).astype(BF16)
            dx_all[pl.ds(my_slot, 1)] = dx_mine[...][None]

            def send(i):
                pltpu.make_async_remote_copy(dx_mine, dx_all.at[my_slot], dxb_send, dxb_recv.at[k],
                                             device_id=peer(lax.rem(me + i, n)), device_id_type=MESH).start()

            each(1, n, send)

    def logits(q):
        return jnp.dot(e[pl.ds(q * SUB, SUB), :], xa[...], preferred_element_type=F32)

    chunks = items // SUB

    def merge(tops, sums):
        top = functools.reduce(jnp.maximum, tops)
        return top, sum(s * jnp.exp2((m - top) * LOG2E) for m, s in zip(tops, sums))

    def exp_sum(ref, m):
        total = jnp.zeros((8, QB), F32)
        for g in range(SUB // 64):
            z = ref[64 * g:64 * g + 64, :].reshape(8, 8, QB)
            total = total + jnp.sum(jnp.exp2((z - m[None]) * LOG2E), axis=0)
        return total

    per_step = -(-(chips - 1) // (2 * BLOCKS - 2))

    def send_rows(step):
        @pl.loop(0, per_step)
        def _(i):
            c = step * per_step + i + 1

            @pl.when(c < chips)
            def _():
                pltpu.make_async_remote_copy(q_ref, q_all.at[my_row], q_sem.at[0], q_sem.at[1],
                                             device_id=peer(lax.rem(chip + c, chips) * 2 + core), device_id_type=MESH).start()

    @pl.loop(0, BLOCKS)
    def _(k):
        xa[0:128, :] = x_all[pl.ds(row0(k), ob)].reshape(QB, 128).T
        xa[128:144, :] = stack_rows([1.0] * 3, 16, QB).astype(BF16)

        m = s = None
        tops, sums = [], []
        for q in range(chunks + 1):
            new, old = (za, zb) if q % 2 == 0 else (zb, za)
            if q < chunks:
                z = logits(q)
                new[...] = z
            if q > 0:
                sums.append(exp_sum(old, tops[len(sums)]))
            if q < chunks:
                tops.append(jnp.max(z.reshape(SUB // 8, 8, QB), axis=0))
            if len(sums) == 4 or q == chunks:
                done = len(sums)
                old_parts = ([m], [s]) if m is not None else ([], [])
                m, s = merge(old_parts[0] + tops[:done], old_parts[1] + sums)
                tops, sums = tops[done:], []
        top = jnp.max(m, axis=0, keepdims=True)
        total = jnp.sum(s * jnp.exp2((m - top) * LOG2E), axis=0, keepdims=True)
        for t in range(2):
            st_send[pl.ds(k * 2 + t, 1)] = jnp.concatenate([top[:, t * 128:(t + 1) * 128], total[:, t * 128:(t + 1) * 128]], axis=0)[None]
        for t in range(2):
            to = stat_owner(k, t, n)

            @pl.when(to != me)
            def _():
                pltpu.make_async_remote_copy(st_send.at[k * 2 + t], st_got.at[me], st_sem.at[0], st_sem.at[1], device_id=peer(to), device_id_type=MESH).start()

            @pl.when(to == me)
            def _():
                st_got[pl.ds(me, 1)] = st_send[pl.ds(k * 2 + t, 1)]

        send_rows(k)
        combine_stats(jnp.where(k == BLOCKS - 1, 2, jnp.where(k < 6, k - 4, -1)))

    drain(lab_all.at[pl.ds(0, n - 1)], lab_sem.at[1])
    swap_q = swap_cores(q_all, swap_sem)

    def grads(k, kept):
        send_rows(BLOCKS + k)

        for t in range(2):
            @pl.when(stat_owner(k, t, n) != me)
            def _():
                drain(st_all.at[0], stb_recv.at[k * 2 + t])

        xb[...] = x_all[pl.ds(row0(k), ob)].reshape(QB, 128)
        xa[0:128, :] = xb[...].T
        top = jnp.concatenate([st_all[k * 2, 0:1, :], st_all[k * 2 + 1, 0:1, :]], axis=1)
        norm = jnp.concatenate([st_all[k * 2, 1:2, :], st_all[k * 2 + 1, 1:2, :]], axis=1) + math.log(n * rows)
        xa[128:144, :] = stack_rows([1.0] * 3 + split3(-top) + split3(-norm), 16, QB).astype(BF16)
        lab = jnp.concatenate([jnp.sum(lab_all[pl.ds(row0(k) + t * half, half)], axis=0) for t in range(2)], axis=1) - me * items
        dxt[...] = jnp.zeros_like(dxt)
        gb[...] = jnp.zeros_like(gb)


        def spread(src, dst, q):
            tsum = t_acc[...]
            for u in range(SUB // 64):
                part = pl.ds(u * 64, 64)
                z = src[part, :]
                idv = ids[part, :]
                hot = jnp.where(jnp.concatenate([idv, idv], axis=1) == lab - q * SUB, 1.0 / (n * rows), 0.0)
                tsum = tsum + jnp.sum((z * hot).reshape(8, 8, QB), axis=0)
                dst[part, :] = (jnp.exp2(z * LOG2E) - hot).astype(BF16)
            t_acc[...] = tsum

        for q in range(chunks + 2):
            if q < chunks:
                (za if q % 2 == 0 else zb)[...] = logits(q)
            if 0 < q <= chunks:
                to = ga if q % 2 else gb
                spread(zb if q % 2 == 0 else za, to if kept is None else keep.at[kept, pl.ds((q - 1) * SUB, SUB)], q - 1)
            if q > 1:
                r = pl.ds((q - 2) * SUB, SUB)
                g = (gb if q % 2 else ga)[...] if kept is None else keep[kept, r, :]
                if kept is None:
                    de_acc[r, :] += jnp.dot(g, xb[...], preferred_element_type=F32)
                dxt[...] += jnp.dot(et[:, r], g, preferred_element_type=F32)

        dx_part[pl.ds(k * ob, ob)] = dxt[...].T.reshape(ob, rows, 128)

        pltpu.make_async_remote_copy(dx_part.at[pl.ds(k * ob + (1 - core) * half, half)], pair.at[pl.ds(k * half, half)], pair_send, pair_recv.at[k],
                                     device_id=peer(chip * 2 + 1 - core), device_id_type=MESH).start()

        @pl.when(k > 0)
        def _():
            flush(k - 1)

        combine_stats(k + 3)

        combine_rows(k - 4)

    pl.loop(0, BLOCKS - KEEP)(lambda k: grads(k, None))
    pl.loop(BLOCKS - KEEP, BLOCKS)(lambda k: grads(k, k - (BLOCKS - KEEP)))

    t_mine[...] = jnp.sum(t_acc[:, 0:128] + t_acc[:, 128:256], axis=0, keepdims=True)
    t_all[pl.ds(me, 1)] = t_mine[...][None]

    def send_t(i):
        pltpu.make_async_remote_copy(t_mine, t_all.at[me], t_sem.at[0], t_sem.at[1], device_id=peer(lax.rem(me + i, n)), device_id_type=MESH).start()

    each(1, n, send_t)

    flush(BLOCKS - 1)
    drain(q_all.at[pl.ds(0, chips - 1)], q_sem.at[1])
    swap_q.start()

    for i in range(KEEP):
        xk[pl.ds(i * QB, QB), :] = x_all[pl.ds(row0(BLOCKS - KEEP + i), ob)].reshape(QB, 128)

    @pl.loop(0, items // 512)
    def _(i):
        r = pl.ds(pl.multiple_of(i * 512, 512), 512)
        g = jnp.concatenate([keep[b, r, :] for b in range(KEEP)], axis=1)
        de_out[r, :] = (de_acc[r, :] + jnp.dot(g, xk[...], preferred_element_type=F32)).astype(BF16)

    out = pltpu.make_async_copy(de_out, de_hbm, out_sem)
    out.start()
    combine_rows(BLOCKS - 4)
    combine_rows(BLOCKS - 3)
    drain(q_all.at[pl.ds(0, chips)], swap_sem.at[1])

    def rows_of(k):
        return q_all[pl.ds(row0(k), ob)].reshape(QB, q_all.shape[-1])

    def pre_act(k):
        pre[pl.ds(k, 1)] = jnp.dot(rows_of(k), w1[...], preferred_element_type=F32)[None]

    def tower(k):
        @pl.when(my_k == k)
        def _():
            if ob > 1:
                drain(dx_all.at[pl.ds(0, ob - 1)], dxb_recv.at[k])

        @pl.when(my_k != k)
        def _():
            drain(dx_all.at[pl.ds(0, ob)], dxb_recv.at[k])

        dx = dx_all[pl.ds(k * ob, ob)].reshape(QB, 128)
        a = pre[k]
        h = jnp.maximum(a, 0.0).astype(BF16)
        acc2[...] += lax.dot_general(h, dx, (((0,), (0,)), ((), ())), preferred_element_type=F32)
        dh = lax.dot_general(dx, w2[...], (((1,), (1,)), ((), ())), preferred_element_type=F32)
        da = jnp.where(a > 0.0, dh, 0.0).astype(BF16)
        acc1[...] += lax.dot_general(rows_of(k), da, (((0,), (0,)), ((), ())), preferred_element_type=F32)

    pl.loop(0, 4)(pre_act)
    combine_rows(BLOCKS - 2)
    combine_rows(BLOCKS - 1)
    pl.loop(4, BLOCKS)(pre_act)
    pl.loop(0, BLOCKS)(tower)
    dw1_ref[...] = acc1[...].astype(BF16)
    dw2_ref[...] = acc2[...].astype(BF16)

    drain(t_all.at[pl.ds(0, n - 1)], t_sem.at[1])
    loss_ref[0] = -jnp.sum(t_all[...]) - math.log(n * rows)

    out.wait()
    swap_q.wait_send()
    swap_x.wait_send()
    drain(x_all.at[pl.ds(0, chips - 1)], x_sem.at[0])
    drain(lab_all.at[pl.ds(0, n - 1)], lab_sem.at[0])
    drain(q_all.at[pl.ds(0, chips - 1)], q_sem.at[0])
    drain(t_all.at[pl.ds(0, n - 1)], t_sem.at[0])
    drain(pair.at[pl.ds(0, BLOCKS * half)], pair_send)

    @pl.when(own_half)
    def _():
        drain(dx_got.at[pl.ds(0, chips - 1)], dx_sem.at[0])

    @pl.when(jnp.logical_not(own_half))
    def _():
        drain(dx_got.at[pl.ds(0, chips)], dx_sem.at[0])

    @pl.when(is_stat)
    def _():
        drain(st_got.at[pl.ds(0, n - 1)], stb_send)
        drain(st_got.at[pl.ds(0, 2 * BLOCKS - 1)], st_sem.at[0])

    @pl.when(jnp.logical_not(is_stat))
    def _():
        drain(st_got.at[pl.ds(0, 2 * BLOCKS)], st_sem.at[0])

    drain(dx_all.at[pl.ds(0, n - 1)], dxb_send)


def store_kernel(pieces, *refs):
    count = len(pieces)
    ins, outs, bufs, in_sem, out_sem = refs[:count], refs[count:2 * count], refs[2 * count:3 * count], refs[-2], refs[-1]
    reads, writes = [], []
    for a, o, v, p in zip(ins, outs, bufs, pieces):
        step = a.shape[0] // p
        for i in range(p):
            part = pl.ds(i * step, step)
            at = len(reads)
            reads.append(pltpu.make_async_copy(a.at[part], v.at[part], in_sem.at[at]))
            writes.append(pltpu.make_async_copy(v.at[part], o.at[part], out_sem.at[at]))
    for c in reads:
        c.start()
    for r, w in zip(reads, writes):
        r.wait()
        w.start()
    for w in writes:
        w.wait()


def store(*arrays):
    pieces = (4, 2, 1)
    any_space = pl.BlockSpec(memory_space=pl.ANY)
    return pl.pallas_call(
        functools.partial(store_kernel, pieces),
        name="store",
        out_shape=tuple(jax.ShapeDtypeStruct(a.shape, a.dtype) for a in arrays),
        in_specs=[any_space] * 3,
        out_specs=(any_space,) * 3,
        scratch_shapes=[pltpu.VMEM(a.shape, a.dtype) for a in arrays] + [DMA((sum(pieces),)), DMA((sum(pieces),))],
        compiler_params=pltpu.CompilerParams(vmem_limit_bytes=60 << 20),
    )(*arrays)


def solution(mesh):
    n = mesh.shape["tp"]

    def local_step(queries, w_first, w_second, catalogue, log_q, labels):
        rows, width = queries.shape
        items = catalogue.shape[0]
        hidden = w_first.shape[1]
        ob = n // BLOCKS
        V, ANY = pl.BlockSpec(memory_space=pltpu.VMEM), pl.BlockSpec(memory_space=pl.ANY)
        S = jax.ShapeDtypeStruct
        M = pltpu.VMEM
        i32 = jnp.int32
        loss, grad_items, grad_first, grad_second = pl.pallas_call(
            functools.partial(kernel, n, rows, items),
            name="two_tower",
            out_shape=(S((1,), F32), S((items, 128), BF16), S((width, hidden), BF16), S((hidden, 128), BF16)),
            in_specs=[V, ANY, ANY, ANY, V, V],
            out_specs=(pl.BlockSpec(memory_space=pltpu.SMEM), ANY, V, V),
            scratch_shapes=[
                M((width, hidden), BF16), M((hidden, 128), BF16), M((items, 256), BF16), M((128, items), BF16), M((SUB, 128), i32),
                M((rows, 128), BF16), M((1, 128), i32), M((n, rows, 128), BF16), M((n, 1, 128), i32), M((n, rows, width), BF16), M((256, QB), BF16), M((QB, 128), BF16), M((SUB, QB), F32), M((SUB, QB), F32), M((SUB, QB), BF16), M((SUB, QB), BF16), M((KEEP, items, QB), BF16), M((KEEP * QB, 128), BF16),
                M((2 * BLOCKS, 2, 128), F32), M((n, 2, 128), F32), M((2, 128), F32), M((2 * BLOCKS, 2, 128), F32), M((items, 128), F32), M((items, 128), BF16), M((128, QB), F32),
                M((n, rows, 128), F32), M((n // 2, rows, 128), F32), M((n // 2, rows, 128), F32), M((n // 2, rows, 128), F32), M((rows, 128), BF16), M((n, rows, 128), BF16),
                M((8, QB), F32), M((1, 128), F32), M((n, 1, 128), F32), M((BLOCKS, QB, hidden), F32), M((width, hidden), F32), M((hidden, 128), F32),
                DMA((3,)), DMA, DMA((2,)), DMA((2,)), DMA((2,)), DMA((2,)), DMA((2,)), DMA((2,)), DMA, DMA((2 * BLOCKS,)), DMA, DMA((BLOCKS,)), DMA((2,)), DMA, DMA((BLOCKS,)), DMA((2,)),
            ],
            compiler_params=pltpu.CompilerParams(collective_id=0, has_side_effects=True, vmem_limit_bytes=60 << 20),
        )(queries, w_first, w_second, catalogue, log_q.reshape(items // 128, 128), labels.reshape(1, rows))
        return (loss,) + tuple(store(grad_items, grad_first, grad_second))

    row_spec = P(("dp", "tp"), None)
    return jax.shard_map(local_step, mesh=mesh, in_specs=(row_spec, P(None, None), P(None, None), P("tp", None), P("tp"), P(("dp", "tp"))), out_specs=(P("dp"), row_spec, P("dp", None), P("dp", None)), check_vma=False)
```

```python
import functools
import math
import jax
import jax.numpy as jnp
from jax import lax
from jax.experimental import pallas as pl
from jax.experimental.pallas import tpu as pltpu
from jax.sharding import PartitionSpec as P

MESH = pl.DeviceIdType.MESH
DMA = pltpu.SemaphoreType.DMA
F32, BF16 = jnp.float32, jnp.bfloat16
LOG2E = 1.4426950408889634
BLOCKS = 8
QB = 256
SUB = 512
KEEP = 1


def peer(index):
    return {"tp": index}


def drain(ref, sem):
    pltpu.make_async_copy(ref, ref, sem).wait()


def slot_of(d, n):
    core, chip = d % 2, d // 2
    if n == 128:
        x, y, z = chip % 4, (chip // 4) % 4, chip // 16
        return ((x + y + z) % 4) * 2 + core, z * 4 + y
    return (chip % 4) * 2 + core, chip // 4


def device_of(k, j, n):
    if n == 128:
        z, y = j // 4, j % 4
        x = (k // 2 + 8 - y - z) % 4
        return ((z * 4 + y) * 4 + x) * 2 + k % 2
    return (j * 4 + k // 2) * 2 + k % 2


def each(first, count, f):
    steps = (count - first) // 4

    @pl.loop(0, steps)
    def _(s):
        for u in range(4):
            f(first + s * 4 + u)

    for i in range(first + steps * 4, count):
        f(i)


def split3(v):
    big = float(jnp.finfo(BF16).max)
    a = jnp.clip(v, -big, big).astype(BF16).astype(F32)
    b = (v - a).astype(BF16).astype(F32)
    return [a, b, v - a - b]


def stack_rows(values, height, width=128):
    at = lax.broadcasted_iota(jnp.int32, (height, width), 0)
    out = jnp.zeros((height, width), F32)
    for i, v in enumerate(values):
        out = jnp.where(at == i, v, out)
    return out


def stat_owner(k, t, n):
    return device_of(5, 2 * k + t, n) if n == 128 else device_of(k, t * (n // BLOCKS // 2), n)


def kernel(n, rows, items,
           q_ref, w1_hbm, w2_hbm, e_hbm, lq_ref, lab_ref,
           loss_ref, de_hbm, dw1_ref, dw2_ref,
           w1, w2, e, et, ids, x_mine, lab_mine, x_all, lab_all, q_all, xa, xb, za, zb, ga, gb, keep, xk,
           st_send, st_got, st_mine, st_all, de_acc, de_out, dxt, dx_part, pair, dx_sum, dx_got, dx_mine, dx_all,
           t_acc, t_mine, t_all, pre, acc1, acc2,
           load_sem, out_sem, x_sem, xs_sem, lab_sem, q_sem, swap_sem, st_sem, stb_send, stb_recv, pair_send, pair_recv, dx_sem, dxb_send, dxb_recv, t_sem):
    me = lax.axis_index("tp")
    ob = n // BLOCKS
    half = ob // 2
    my_k, my_j = slot_of(me, n)
    my_slot = my_k * ob + my_j
    core, chip, chips = me % 2, me // 2, n // 2
    my_row = core * chips + (my_k // 2) * ob + my_j

    if n == 128:
        is_stat, stat_k, stat_t = my_k == 5, my_j // 2, my_j % 2
    else:
        is_stat, stat_k, stat_t = my_j % half == 0, my_k, my_j // half

    def row0(k):
        return (k % 2) * chips + (k // 2) * ob

    def swap_cores(ref, sem):
        part = ref.at[pl.ds(core * chips, chips)]
        return pltpu.make_async_remote_copy(part, part, sem.at[0], sem.at[1], device_id=peer(chip * 2 + 1 - core), device_id_type=MESH)

    loads = [pltpu.make_async_copy(a, b, load_sem.at[i]) for i, (a, b) in enumerate(((w1_hbm, w1), (w2_hbm, w2), (e_hbm, e.at[:, 0:128])))]
    for c in loads:
        c.start()
    barrier = pltpu.get_barrier_semaphore()

    each(1, n, lambda k: pl.semaphore_signal(barrier, inc=1, device_id=peer(lax.rem(me + k, n)), device_id_type=MESH))

    loads[0].wait()
    loads[1].wait()
    hid = jnp.maximum(jnp.dot(q_ref[...], w1[...], preferred_element_type=F32), 0.0).astype(BF16)
    x_mine[...] = jnp.dot(hid, w2[...], preferred_element_type=F32).astype(BF16)
    lanes = lax.broadcasted_iota(jnp.int32, (1, 128), 1)
    wide = jnp.concatenate([lab_ref[...]] * (128 // rows), axis=1) if rows < 128 else lab_ref[...]
    lab_mine[...] = jnp.where(lanes // rows == my_j % half, wide, 0)
    x_all[pl.ds(my_row, 1)] = x_mine[...][None]
    lab_all[pl.ds(my_row, 1)] = lab_mine[...][None]
    q_all[pl.ds(my_row, 1)] = q_ref[...][None]
    loads[2].wait()

    @pl.loop(0, items // 1024)
    def _(i):
        parts = split3(-lq_ref[pl.ds(pl.multiple_of(i * 8, 8), 8), :])
        for u in range(8):
            r = pl.multiple_of(i * 1024 + u * 128, 128)
            extra = stack_rows([p[u:u + 1, :] for p in parts] + [1.0] * 6, 16)
            e[pl.ds(r, 128), 128:256] = jnp.concatenate([extra, jnp.zeros((112, 128), F32)], axis=0).T.astype(BF16)
            et[:, pl.ds(r, 128)] = e[pl.ds(r, 128), 0:128].T
            de_acc[pl.ds(r, 128), :] = jnp.zeros((128, 128), F32)

    ids[...] = lax.broadcasted_iota(jnp.int32, (SUB, 128), 0)
    xa[144:256, :] = jnp.zeros((112, QB), BF16)
    t_acc[...] = jnp.zeros_like(t_acc)
    acc1[...] = jnp.zeros_like(acc1)
    acc2[...] = jnp.zeros_like(acc2)
    pl.semaphore_wait(barrier, n - 1)

    def send_x(k):
        to = peer(lax.rem(chip + k, chips) * 2 + core)
        pltpu.make_async_remote_copy(x_mine, x_all.at[my_row], x_sem.at[0], x_sem.at[1], device_id=to, device_id_type=MESH).start()

    def send_labels(k):
        to = peer(lax.rem(me + k, n))
        pltpu.make_async_remote_copy(lab_mine, lab_all.at[my_row], lab_sem.at[0], lab_sem.at[1], device_id=to, device_id_type=MESH).start()

    each(1, chips, send_x)
    each(1, n, send_labels)
    drain(x_all.at[pl.ds(0, chips - 1)], x_sem.at[1])
    swap_x = swap_cores(x_all, xs_sem)
    swap_x.start()
    drain(x_all.at[pl.ds(0, chips)], xs_sem.at[1])


    def combine_stats(k):
        @pl.when(jnp.logical_and(is_stat, stat_k == k))
        def _():
            drain(st_got.at[pl.ds(0, n - 1)], st_sem.at[1])
            top = jnp.max(st_got[:, 0:1, :], axis=0)
            total = jnp.sum(st_got[:, 1:2, :] * jnp.exp(st_got[:, 0:1, :] - top[None]), axis=0)
            st_mine[...] = jnp.concatenate([top, jnp.log(total)], axis=0)
            st_all[pl.ds(k * 2 + stat_t, 1)] = st_mine[...][None]

            def send(i):
                pltpu.make_async_remote_copy(st_mine, st_all.at[k * 2 + stat_t], stb_send, stb_recv.at[k * 2 + stat_t],
                                             device_id=peer(lax.rem(me + i, n)), device_id_type=MESH).start()

            each(1, n, send)

    def flush(k):
        drain(pair.at[pl.ds(0, half)], pair_recv.at[k])
        dx_sum[pl.ds(k * half, half)] = dx_part[pl.ds(k * ob + core * half, half)] + pair[pl.ds(k * half, half)]

        @pl.loop(0, half)
        def _(j):
            to = device_of(k, core * half + j, n)

            @pl.when(to != me)
            def _():
                pltpu.make_async_remote_copy(dx_sum.at[k * half + j], dx_got.at[chip], dx_sem.at[0], dx_sem.at[1], device_id=peer(to), device_id_type=MESH).start()

            @pl.when(to == me)
            def _():
                dx_got[pl.ds(chip, 1)] = dx_sum[pl.ds(k * half + j, 1)]

    own_half = my_j // half == core

    def combine_rows(k):
        @pl.when(my_k == k)
        def _():
            @pl.when(own_half)
            def _():
                drain(dx_got.at[pl.ds(0, chips - 1)], dx_sem.at[1])

            @pl.when(jnp.logical_not(own_half))
            def _():
                drain(dx_got.at[pl.ds(0, chips)], dx_sem.at[1])

            dx_mine[...] = jnp.sum(dx_got[...], axis=0).astype(BF16)
            dx_all[pl.ds(my_slot, 1)] = dx_mine[...][None]

            def send(i):
                pltpu.make_async_remote_copy(dx_mine, dx_all.at[my_slot], dxb_send, dxb_recv.at[k],
                                             device_id=peer(lax.rem(me + i, n)), device_id_type=MESH).start()

            each(1, n, send)

    def logits(q):
        return jnp.dot(e[pl.ds(q * SUB, SUB), :], xa[...], preferred_element_type=F32)

    chunks = items // SUB

    def merge(tops, sums):
        top = functools.reduce(jnp.maximum, tops)
        return top, sum(s * jnp.exp2((m - top) * LOG2E) for m, s in zip(tops, sums))

    def exp_sum(ref, m):
        total = jnp.zeros((8, QB), F32)
        for g in range(SUB // 64):
            z = ref[64 * g:64 * g + 64, :].reshape(8, 8, QB)
            total = total + jnp.sum(jnp.exp2((z - m[None]) * LOG2E), axis=0)
        return total

    def send_rows(first, count):
        @pl.loop(0, count)
        def _(i):
            c = first + i + 1

            @pl.when(c < chips)
            def _():
                pltpu.make_async_remote_copy(q_ref, q_all.at[my_row], q_sem.at[0], q_sem.at[1],
                                             device_id=peer(lax.rem(chip + c, chips) * 2 + core), device_id_type=MESH).start()

    @pl.loop(0, BLOCKS)
    def _(k):
        xa[0:128, :] = x_all[pl.ds(row0(k), ob)].reshape(QB, 128).T
        xa[128:144, :] = stack_rows([1.0] * 3, 16, QB).astype(BF16)

        m = s = None
        tops, sums = [], []
        for q in range(chunks + 1):
            new, old = (za, zb) if q % 2 == 0 else (zb, za)
            if q < chunks:
                z = logits(q)
                new[...] = z
            if q > 0:
                sums.append(exp_sum(old, tops[len(sums)]))
            if q < chunks:
                tops.append(jnp.max(z.reshape(SUB // 8, 8, QB), axis=0))
            if len(sums) == 4 or q == chunks:
                done = len(sums)
                old_parts = ([m], [s]) if m is not None else ([], [])
                m, s = merge(old_parts[0] + tops[:done], old_parts[1] + sums)
                tops, sums = tops[done:], []
        top = jnp.max(m, axis=0, keepdims=True)
        total = jnp.sum(s * jnp.exp2((m - top) * LOG2E), axis=0, keepdims=True)
        for t in range(2):
            st_send[pl.ds(k * 2 + t, 1)] = jnp.concatenate([top[:, t * 128:(t + 1) * 128], total[:, t * 128:(t + 1) * 128]], axis=0)[None]
        for t in range(2):
            to = stat_owner(k, t, n)

            @pl.when(to != me)
            def _():
                pltpu.make_async_remote_copy(st_send.at[k * 2 + t], st_got.at[me], st_sem.at[0], st_sem.at[1], device_id=peer(to), device_id_type=MESH).start()

            @pl.when(to == me)
            def _():
                st_got[pl.ds(me, 1)] = st_send[pl.ds(k * 2 + t, 1)]

        send_rows(2 * k, 2)
        combine_stats(k - 4)

    drain(lab_all.at[pl.ds(0, n - 1)], lab_sem.at[1])
    swap_q = swap_cores(q_all, swap_sem)

    late = max(-(-(chips - 1 - 2 * BLOCKS) // (BLOCKS - 2)), 1)

    def grads(k, kept):
        send_rows(2 * BLOCKS + k * late, late)

        for t in range(2):
            @pl.when(stat_owner(k, t, n) != me)
            def _():
                drain(st_all.at[0], stb_recv.at[k * 2 + t])

        xb[...] = x_all[pl.ds(row0(k), ob)].reshape(QB, 128)
        xa[0:128, :] = xb[...].T
        top = jnp.concatenate([st_all[k * 2, 0:1, :], st_all[k * 2 + 1, 0:1, :]], axis=1)
        norm = jnp.concatenate([st_all[k * 2, 1:2, :], st_all[k * 2 + 1, 1:2, :]], axis=1) + math.log(n * rows)
        xa[128:144, :] = stack_rows([1.0] * 3 + split3(-top) + split3(-norm), 16, QB).astype(BF16)
        lab = jnp.concatenate([jnp.sum(lab_all[pl.ds(row0(k) + t * half, half)], axis=0) for t in range(2)], axis=1) - me * items
        dxt[...] = jnp.zeros_like(dxt)
        gb[...] = jnp.zeros_like(gb)


        def spread(src, dst, q):
            tsum = t_acc[...]
            for u in range(SUB // 64):
                part = pl.ds(u * 64, 64)
                z = src[part, :]
                idv = ids[part, :]
                hot = jnp.where(jnp.concatenate([idv, idv], axis=1) == lab - q * SUB, 1.0 / (n * rows), 0.0)
                tsum = tsum + jnp.sum((z * hot).reshape(8, 8, QB), axis=0)
                dst[part, :] = (jnp.exp2(z * LOG2E) - hot).astype(BF16)
            t_acc[...] = tsum

        for q in range(chunks + 2):
            if q < chunks:
                (za if q % 2 == 0 else zb)[...] = logits(q)
            if 0 < q <= chunks:
                to = ga if q % 2 else gb
                spread(zb if q % 2 == 0 else za, to if kept is None else keep.at[kept, pl.ds((q - 1) * SUB, SUB)], q - 1)
            if q > 1:
                r = pl.ds((q - 2) * SUB, SUB)
                g = (gb if q % 2 else ga)[...] if kept is None else keep[kept, r, :]
                if kept is None:
                    de_acc[r, :] += jnp.dot(g, xb[...], preferred_element_type=F32)
                dxt[...] += jnp.dot(et[:, r], g, preferred_element_type=F32)

        dx_part[pl.ds(k * ob, ob)] = dxt[...].T.reshape(ob, rows, 128)

        pltpu.make_async_remote_copy(dx_part.at[pl.ds(k * ob + (1 - core) * half, half)], pair.at[pl.ds(k * half, half)], pair_send, pair_recv.at[k],
                                     device_id=peer(chip * 2 + 1 - core), device_id_type=MESH).start()

        @pl.when(k > 0)
        def _():
            flush(k - 1)

        combine_stats(k + 4)

        combine_rows(k - 4)

    pl.loop(0, BLOCKS - KEEP)(lambda k: grads(k, None))
    pl.loop(BLOCKS - KEEP, BLOCKS)(lambda k: grads(k, k - (BLOCKS - KEEP)))

    t_mine[...] = jnp.sum(t_acc[:, 0:128] + t_acc[:, 128:256], axis=0, keepdims=True)
    t_all[pl.ds(me, 1)] = t_mine[...][None]

    def send_t(i):
        pltpu.make_async_remote_copy(t_mine, t_all.at[me], t_sem.at[0], t_sem.at[1], device_id=peer(lax.rem(me + i, n)), device_id_type=MESH).start()

    each(1, n, send_t)

    flush(BLOCKS - 1)
    drain(q_all.at[pl.ds(0, chips - 1)], q_sem.at[1])
    swap_q.start()

    for i in range(KEEP):
        xk[pl.ds(i * QB, QB), :] = x_all[pl.ds(row0(BLOCKS - KEEP + i), ob)].reshape(QB, 128)

    @pl.loop(0, items // 512)
    def _(i):
        r = pl.ds(pl.multiple_of(i * 512, 512), 512)
        g = jnp.concatenate([keep[b, r, :] for b in range(KEEP)], axis=1)
        de_out[r, :] = (de_acc[r, :] + jnp.dot(g, xk[...], preferred_element_type=F32)).astype(BF16)

    out = pltpu.make_async_copy(de_out, de_hbm, out_sem)
    out.start()
    combine_rows(BLOCKS - 4)
    combine_rows(BLOCKS - 3)
    drain(q_all.at[pl.ds(0, chips)], swap_sem.at[1])

    def rows_of(k):
        return q_all[pl.ds(row0(k), ob)].reshape(QB, q_all.shape[-1])

    def pre_act(k):
        pre[pl.ds(k, 1)] = jnp.dot(rows_of(k), w1[...], preferred_element_type=F32)[None]

    def tower(k):
        @pl.when(my_k == k)
        def _():
            if ob > 1:
                drain(dx_all.at[pl.ds(0, ob - 1)], dxb_recv.at[k])

        @pl.when(my_k != k)
        def _():
            drain(dx_all.at[pl.ds(0, ob)], dxb_recv.at[k])

        dx = dx_all[pl.ds(k * ob, ob)].reshape(QB, 128)
        a = pre[k]
        h = jnp.maximum(a, 0.0).astype(BF16)
        acc2[...] += lax.dot_general(h, dx, (((0,), (0,)), ((), ())), preferred_element_type=F32)
        dh = lax.dot_general(dx, w2[...], (((1,), (1,)), ((), ())), preferred_element_type=F32)
        da = jnp.where(a > 0.0, dh, 0.0).astype(BF16)
        acc1[...] += lax.dot_general(rows_of(k), da, (((0,), (0,)), ((), ())), preferred_element_type=F32)

    pl.loop(0, 2)(pre_act)
    combine_rows(BLOCKS - 2)
    combine_rows(BLOCKS - 1)
    pl.loop(2, BLOCKS)(pre_act)
    pl.loop(0, BLOCKS)(tower)
    dw1_ref[...] = acc1[...].astype(BF16)
    dw2_ref[...] = acc2[...].astype(BF16)

    drain(t_all.at[pl.ds(0, n - 1)], t_sem.at[1])
    loss_ref[0] = -jnp.sum(t_all[...]) - math.log(n * rows)

    out.wait()
    swap_q.wait_send()
    swap_x.wait_send()
    drain(x_all.at[pl.ds(0, chips - 1)], x_sem.at[0])
    drain(lab_all.at[pl.ds(0, n - 1)], lab_sem.at[0])
    drain(q_all.at[pl.ds(0, chips - 1)], q_sem.at[0])
    drain(t_all.at[pl.ds(0, n - 1)], t_sem.at[0])
    drain(pair.at[pl.ds(0, BLOCKS * half)], pair_send)

    @pl.when(own_half)
    def _():
        drain(dx_got.at[pl.ds(0, chips - 1)], dx_sem.at[0])

    @pl.when(jnp.logical_not(own_half))
    def _():
        drain(dx_got.at[pl.ds(0, chips)], dx_sem.at[0])

    @pl.when(is_stat)
    def _():
        drain(st_got.at[pl.ds(0, n - 1)], stb_send)
        drain(st_got.at[pl.ds(0, 2 * BLOCKS - 1)], st_sem.at[0])

    @pl.when(jnp.logical_not(is_stat))
    def _():
        drain(st_got.at[pl.ds(0, 2 * BLOCKS)], st_sem.at[0])

    drain(dx_all.at[pl.ds(0, n - 1)], dxb_send)


def store_kernel(pieces, *refs):
    count = len(pieces)
    ins, outs, bufs, in_sem, out_sem = refs[:count], refs[count:2 * count], refs[2 * count:3 * count], refs[-2], refs[-1]
    reads, writes = [], []
    for a, o, v, p in zip(ins, outs, bufs, pieces):
        step = a.shape[0] // p
        for i in range(p):
            part = pl.ds(i * step, step)
            at = len(reads)
            reads.append(pltpu.make_async_copy(a.at[part], v.at[part], in_sem.at[at]))
            writes.append(pltpu.make_async_copy(v.at[part], o.at[part], out_sem.at[at]))
    for c in reads:
        c.start()
    for r, w in zip(reads, writes):
        r.wait()
        w.start()
    for w in writes:
        w.wait()


def store(*arrays):
    pieces = (4, 2, 1)
    any_space = pl.BlockSpec(memory_space=pl.ANY)
    return pl.pallas_call(
        functools.partial(store_kernel, pieces),
        name="store",
        out_shape=tuple(jax.ShapeDtypeStruct(a.shape, a.dtype) for a in arrays),
        in_specs=[any_space] * 3,
        out_specs=(any_space,) * 3,
        scratch_shapes=[pltpu.VMEM(a.shape, a.dtype) for a in arrays] + [DMA((sum(pieces),)), DMA((sum(pieces),))],
        compiler_params=pltpu.CompilerParams(vmem_limit_bytes=60 << 20),
    )(*arrays)


def solution(mesh):
    n = mesh.shape["tp"]

    def local_step(queries, w_first, w_second, catalogue, log_q, labels):
        rows, width = queries.shape
        items = catalogue.shape[0]
        hidden = w_first.shape[1]
        ob = n // BLOCKS
        V, ANY = pl.BlockSpec(memory_space=pltpu.VMEM), pl.BlockSpec(memory_space=pl.ANY)
        S = jax.ShapeDtypeStruct
        M = pltpu.VMEM
        i32 = jnp.int32
        loss, grad_items, grad_first, grad_second = pl.pallas_call(
            functools.partial(kernel, n, rows, items),
            name="two_tower",
            out_shape=(S((1,), F32), S((items, 128), BF16), S((width, hidden), BF16), S((hidden, 128), BF16)),
            in_specs=[V, ANY, ANY, ANY, V, V],
            out_specs=(pl.BlockSpec(memory_space=pltpu.SMEM), ANY, V, V),
            scratch_shapes=[
                M((width, hidden), BF16), M((hidden, 128), BF16), M((items, 256), BF16), M((128, items), BF16), M((SUB, 128), i32),
                M((rows, 128), BF16), M((1, 128), i32), M((n, rows, 128), BF16), M((n, 1, 128), i32), M((n, rows, width), BF16), M((256, QB), BF16), M((QB, 128), BF16), M((SUB, QB), F32), M((SUB, QB), F32), M((SUB, QB), BF16), M((SUB, QB), BF16), M((KEEP, items, QB), BF16), M((KEEP * QB, 128), BF16),
                M((2 * BLOCKS, 2, 128), F32), M((n, 2, 128), F32), M((2, 128), F32), M((2 * BLOCKS, 2, 128), F32), M((items, 128), F32), M((items, 128), BF16), M((128, QB), F32),
                M((n, rows, 128), F32), M((n // 2, rows, 128), F32), M((n // 2, rows, 128), F32), M((n // 2, rows, 128), F32), M((rows, 128), BF16), M((n, rows, 128), BF16),
                M((8, QB), F32), M((1, 128), F32), M((n, 1, 128), F32), M((BLOCKS, QB, hidden), F32), M((width, hidden), F32), M((hidden, 128), F32),
                DMA((3,)), DMA, DMA((2,)), DMA((2,)), DMA((2,)), DMA((2,)), DMA((2,)), DMA((2,)), DMA, DMA((2 * BLOCKS,)), DMA, DMA((BLOCKS,)), DMA((2,)), DMA, DMA((BLOCKS,)), DMA((2,)),
            ],
            compiler_params=pltpu.CompilerParams(collective_id=0, has_side_effects=True, vmem_limit_bytes=60 << 20),
        )(queries, w_first, w_second, catalogue, log_q.reshape(items // 128, 128), labels.reshape(1, rows))
        return (loss,) + tuple(store(grad_items, grad_first, grad_second))

    row_spec = P(("dp", "tp"), None)
    return jax.shard_map(local_step, mesh=mesh, in_specs=(row_spec, P(None, None), P(None, None), P("tp", None), P("tp"), P(("dp", "tp"))), out_specs=(P("dp"), row_spec, P("dp", None), P("dp", None)), check_vma=False)
```
